32 devices in a mesh: dp: 4 (over y, z), tp: 8 (over x, core).
Axes of the slice: x: 4, y: 2, z: 2, core: 2. Of those that a mesh axis runs over, the one named last changes fastest.
The devices are a block of a 4x4x8 slice.
Arguments:
- x: bfloat16 [512, 4096], P('dp'), parts along dimension 0
- g_attn: bfloat16 [2, 4096], replicated
- w_qkv: bfloat16 [2, 4096, 6144], P(None, None, 'tp')
- w_o: bfloat16 [2, 4096, 4096], P(None, 'tp')
- g_mlp: bfloat16 [2, 4096], replicated
- w_gate: bfloat16 [2, 4096, 14336], P(None, None, 'tp')
- w_up: bfloat16 [2, 4096, 14336], P(None, None, 'tp')
- w_down: bfloat16 [2, 14336, 4096], P(None, 'tp')
- k_cache: bfloat16 [2, 512, 128, 8, 128], P(None, 'dp', None, 'tp'), parts along dimension 1
- v_cache: bfloat16 [2, 512, 128, 8, 128], P(None, 'dp', None, 'tp'), parts along dimension 1
- lengths: int32 [512], P('dp'), parts along dimension 0
Outputs:
- output: bfloat16 [512, 4096], P('dp'), parts along dimension 0
There are 4 independent parts. The reference program is written for one: setup_inputs(seed, part) draws one part's arguments, and reference() takes and returns one part's arrays. A program takes and returns all parts, laid end to end along the dimension named above; an argument that names none is the same for every part.
All inputs are finite; a program needn't handle non-finite values.
Results may differ from the reference program's by a relative error of at most 0.02.
Values are sent between devices in bfloat16 or wider.
A program may use at most 768 MiB of HBM per device.

```python
import jax
import jax.numpy as jnp
from jax import lax

D = 4096
HEADS = 32
KV_HEADS = 8
HEAD = 128
FF = 14336
BATCH = 128
SEQ = 128
LAYERS = 2
TP = 8

GROUP = HEADS // KV_HEADS
QKV = (HEADS + 2 * KV_HEADS) * HEAD
EPS = 1e-5
ROPE_THETA = 500000.0


def setup_inputs(seed: int = 0, part: int = 0) -> dict:
    key = jax.random.PRNGKey(seed)
    ks = jax.random.split(key, 8)
    kp = jax.random.split(jax.random.fold_in(ks[7], part), 5)

    def normal(k, shape, scale):
        return (scale * jax.random.normal(k, shape, jnp.float32)).astype(jnp.bfloat16)

    def gain(k):
        return jax.random.uniform(k, (LAYERS, D), jnp.float32, 0.7, 1.3).astype(jnp.bfloat16)

    g_attn = gain(ks[0])
    w_qkv = normal(ks[1], (LAYERS, D, QKV), D ** -0.5)
    w_o = normal(ks[2], (LAYERS, HEADS * HEAD, D), (HEADS * HEAD) ** -0.5)
    g_mlp = gain(ks[3])
    w_gate = normal(ks[4], (LAYERS, D, FF), D ** -0.5)
    w_up = normal(ks[5], (LAYERS, D, FF), D ** -0.5)
    w_down = normal(ks[6], (LAYERS, FF, D), FF ** -0.5)
    x = normal(kp[0], (BATCH, D), 1.0)
    lengths = jax.random.randint(kp[1], (BATCH,), 1, SEQ, dtype=jnp.int32)
    shape = (LAYERS, BATCH, SEQ, KV_HEADS, HEAD)
    stale = jnp.arange(SEQ)[None, None, :, None, None] >= lengths[None, :, None, None, None]
    k_cache = (2.0 * jax.random.normal(kp[2], shape, jnp.float32)).astype(jnp.bfloat16)
    mu = jax.random.normal(kp[3], (LAYERS, BATCH, 1, KV_HEADS, HEAD), jnp.float32)
    v_cache = 0.7 * mu + jax.random.normal(kp[4], shape, jnp.float32)
    v_cache = jnp.where(stale, v_cache + 2.0, v_cache).astype(jnp.bfloat16)
    return {'x': x, 'g_attn': g_attn, 'w_qkv': w_qkv, 'w_o': w_o, 'g_mlp': g_mlp,
            'w_gate': w_gate, 'w_up': w_up, 'w_down': w_down,
            'k_cache': k_cache, 'v_cache': v_cache, 'lengths': lengths}


def _rmsnorm(x, g):
    xf = x.astype(jnp.float32)
    r = lax.rsqrt(jnp.mean(xf * xf, axis=-1, keepdims=True) + EPS)
    return (xf * r * g.astype(jnp.float32)).astype(jnp.bfloat16)


def _rope(t, pos):
    half = HEAD // 2
    inv = ROPE_THETA ** (-jnp.arange(half, dtype=jnp.float32) * 2.0 / HEAD)
    ang = pos.astype(jnp.float32)[:, None] * inv[None, :]
    shape = (pos.shape[0],) + (1,) * (t.ndim - 2) + (half,)
    c = jnp.cos(ang).reshape(shape)
    s = jnp.sin(ang).reshape(shape)
    tf = t.astype(jnp.float32)
    t1, t2 = tf[..., :half], tf[..., half:]
    return jnp.concatenate([t1 * c - t2 * s, t2 * c + t1 * s], axis=-1).astype(jnp.bfloat16)


def _attend(q, k_new, v_new, kc, vc, length):
    scale = HEAD ** -0.5
    qf = q.astype(jnp.float32)
    s_c = jnp.einsum('jgd,sjd->jgs', qf, kc.astype(jnp.float32)) * scale
    s_c = jnp.where(jnp.arange(SEQ)[None, None, :] < length, s_c, -jnp.inf)
    s_n = jnp.einsum('jgd,jd->jg', qf, k_new.astype(jnp.float32)) * scale
    m = jnp.maximum(jnp.max(s_c, axis=-1), s_n)
    p_c = jnp.exp(s_c - m[..., None])
    p_n = jnp.exp(s_n - m)
    den = jnp.sum(p_c, axis=-1) + p_n
    o = jnp.einsum('jgs,sjd->jgd', p_c.astype(jnp.bfloat16).astype(jnp.float32), vc.astype(jnp.float32))
    o = o + p_n[..., None] * v_new.astype(jnp.float32)[:, None, :]
    return o / den[..., None]


def _row_parallel(a, w):
    n = w.shape[0] // TP
    return sum(jnp.dot(a[:, i * n:(i + 1) * n], w[i * n:(i + 1) * n], preferred_element_type=jnp.float32)
               .astype(jnp.bfloat16).astype(jnp.float32) for i in range(TP))


def _layer(x, lengths, g1, wqkv, wo, g2, wg, wu, wd, kc, vc):
    a = _rmsnorm(x, g1)
    qkv = jnp.dot(a, wqkv, preferred_element_type=jnp.float32).astype(jnp.bfloat16)
    qkv = qkv.reshape(BATCH, KV_HEADS, GROUP + 2, HEAD)
    q = _rope(qkv[:, :, :GROUP], lengths)
    k = _rope(qkv[:, :, GROUP], lengths)
    v = qkv[:, :, GROUP + 1]
    att = lax.map(lambda t: _attend(*t), (q, k, v, kc, vc, lengths))
    att = att.astype(jnp.bfloat16).reshape(BATCH, HEADS * HEAD)
    h = (x.astype(jnp.float32) + _row_parallel(att, wo)).astype(jnp.bfloat16)
    b = _rmsnorm(h, g2)
    gate = jnp.dot(b, wg, preferred_element_type=jnp.float32)
    up = jnp.dot(b, wu, preferred_element_type=jnp.float32)
    act = (jax.nn.silu(gate) * up).astype(jnp.bfloat16)
    return (h.astype(jnp.float32) + _row_parallel(act, wd)).astype(jnp.bfloat16)


def reference(x, g_attn, w_qkv, w_o, g_mlp, w_gate, w_up, w_down, k_cache, v_cache, lengths):
    def body(h, p):
        return _layer(h, lengths, *p), None
    y, _ = lax.scan(body, x, (g_attn, w_qkv, w_o, g_mlp, w_gate, w_up, w_down, k_cache, v_cache))
    return y
```

```python
import functools

import jax
import jax.numpy as jnp
import numpy as np
from jax import lax
from jax.experimental import pallas as pl
from jax.experimental.pallas import tpu as pltpu
from jax.sharding import PartitionSpec as P

EPS = 1e-5
ROPE_THETA = 500000.0
F32 = jnp.float32
BF16 = jnp.bfloat16
SLOTS = 8
SLOTS_PER_STEP = 2
RS_ORDER = (2, 1, 3, 0)
AG_ORDER = (0, 3, 1, 2)


def _dot(a, b):
    return jnp.dot(a, b, preferred_element_type=F32)


def _dot_nt(a, b):
    return lax.dot_general(a, b, (((1,), (1,)), ((), ())), preferred_element_type=F32)


def _kernel(dims, x_hbm, ga_ref, wqkv_hbm, wo_hbm, gm_ref, wg_hbm, wu_hbm, wd_hbm, kc_hbm, vc_hbm, len_ref, inv_ref,
            y_hbm,
            wq, wo, wg, wu, wd, kv, hbuf, abuf, part, pair_in, relay_in, rs_in, sown, pool, act, lrow, cosb, sinb, att,
            s_x, s_q, s_o, s_g, s_u, s_d, s_kv, s_y,
            pr_s, pr_r, rl_s, rl_r, rs_s, rs_r, ag_s, ag_r, ad_s, ad_r):
    L, n, D, NQ, KO, F, S, hd, R = dims
    NB = 2 * R
    BW = D // NB
    PW = BW // 2
    grp = KO // hd
    T = n // SLOTS
    LW = 128
    NR = n * grp
    qrow, krow, vrow, arow, prow = (pool.at[pl.ds(i * NR, NR)] for i in range(5))
    tp = lax.axis_index("tp")
    x = tp // 2
    c = tp % 2
    right = {"tp": ((x + 1) % R) * 2 + c}
    left = {"tp": ((x + R - 1) % R) * 2 + c}
    partner = {"tp": x * 2 + (1 - c)}
    MESH = pl.DeviceIdType.MESH

    def chip(off):
        return (x + off) % R

    def cols(start, size):
        return pl.ds(pl.multiple_of(start, 128), size)

    def rows(start, size):
        return pl.ds(pl.multiple_of(start, 128), size)

    def cp_x(p):
        return pltpu.make_async_copy(x_hbm.at[:, cols(p * PW, PW)], hbuf.at[p], s_x.at[p])

    def cp_q(l, j):
        return pltpu.make_async_copy(wqkv_hbm.at[l, rows(j * BW, BW), :], wq.at[rows(j * BW, BW), :], s_q.at[j])

    def cp_o(l, j):
        return pltpu.make_async_copy(wo_hbm.at[l, :, cols(j * BW, BW)], wo.at[:, cols(j * BW, BW)], s_o.at[j])

    def cp_g(l, j):
        return pltpu.make_async_copy(wg_hbm.at[l, rows(j * BW, BW), :], wg.at[rows(j * BW, BW), :], s_g.at[j])

    def cp_u(l, j):
        return pltpu.make_async_copy(wu_hbm.at[l, rows(j * BW, BW), :], wu.at[rows(j * BW, BW), :], s_u.at[j])

    def cp_d(l, j):
        return pltpu.make_async_copy(wd_hbm.at[l, :, cols(j * BW, BW)], wd.at[:, cols(j * BW, BW)], s_d.at[j])

    def cp_k(l, s):
        return pltpu.make_async_copy(kc_hbm.at[l, pl.ds(s * T, T)], kv.at[s], s_kv.at[s])

    def cp_v(l, s):
        return pltpu.make_async_copy(vc_hbm.at[l, pl.ds(s * T, T)], kv.at[s], s_kv.at[s])

    def blocks(order):
        return [cc * R + chip(o) for o in order for cc in range(2)]

    barrier = pltpu.get_barrier_semaphore()
    for d in (partner, right, left):
        pl.semaphore_signal(barrier, inc=1, device_id=d, device_id_type=MESH)

    for p in range(2 * NB):
        cp_x(p).start()
    for j in blocks(AG_ORDER):
        cp_q(0, j).start()
    for s in range(SLOTS):
        cp_k(0, s).start()
    for j in range(NB):
        cp_o(0, j).start()

    lcol = jnp.broadcast_to(len_ref[...].astype(F32), (hd, n)).T
    ang = lcol * inv_ref[...]
    lane = lax.broadcasted_iota(jnp.int32, (n, hd), 1)
    cosb[...] = jnp.cos(ang)
    sn = jnp.sin(ang)
    sinb[...] = jnp.where(lane < hd // 2, -sn, sn)
    for g in range(grp):
        lrow[pl.ds(g, n, stride=grp), :] = lcol

    for p in range(2 * NB):
        cp_x(p).wait()

    def gain(ref, l, p):
        g = ref[0:1, cols(p * PW, PW)]
        for i in range(1, L):
            g = jnp.where(l == i, ref[i:i + 1, cols(p * PW, PW)].astype(F32), g.astype(F32))
        return g.astype(F32)

    def norm(l, ref):
        def sq(p, s):
            v = hbuf[p].astype(F32)
            return s + v * v
        s = lax.fori_loop(0, 2 * NB, sq, jnp.zeros((n, PW), F32))
        r = lax.rsqrt(jnp.sum(s, axis=-1, keepdims=True) * (1.0 / D) + EPS)

        def put(p, carry):
            abuf[p] = (hbuf[p].astype(F32) * r * gain(ref, l, p)).astype(BF16)
            return carry
        lax.fori_loop(0, 2 * NB, put, 0)

    def ag_chip(i):
        return chip(jnp.where(i == 0, AG_ORDER[0], jnp.where(i == 1, AG_ORDER[1], jnp.where(i == 2, AG_ORDER[2], AG_ORDER[3]))))

    def group_dot(w, b, n0, nw):
        s = None
        for cc in range(2):
            for h in range(2):
                d = _dot(abuf[cc * NB + b * 2 + h], w[rows((cc * R + b) * BW + h * PW, PW), n0:n0 + nw])
                s = d if s is None else s + d
        return s

    def unit(i):
        return pl.ds(i * n, n)

    def accumulate(u, d):
        for k in range(d.shape[1] // LW):
            pool[unit(u + k), :] += d[:, k * LW:(k + 1) * LW]

    def tiles(width):
        t = []
        n0 = 0
        while n0 < width:
            t.append((n0, min(256, width - n0)))
            n0 += 256
        return t

    def remote(src, dst, ss, rs, dev):
        return pltpu.make_async_remote_copy(src_ref=src, dst_ref=dst, send_sem=ss, recv_sem=rs, device_id=dev,
                                            device_id_type=MESH)

    def all_reduce(block, wait_w):
        pair = []
        for i, off in enumerate(RS_ORDER):
            j = (1 - c) * R + chip(off)
            wait_w(j)
            o = block(j).astype(BF16)
            part[j, 0] = o[:, :PW]
            part[j, 1] = o[:, PW:]
            d = remote(part.at[j], pair_in.at[i], pr_s.at[i], pr_r.at[i], partner)
            d.start()
            pair.append(d)
        sends = []
        for i, off in enumerate(RS_ORDER):
            j = c * R + chip(off)
            wait_w(j)
            o = block(j).astype(BF16).astype(F32)
            pair[i].wait_recv()
            s0 = o[:, :PW] + pair_in[i, 0].astype(F32)
            s1 = o[:, PW:] + pair_in[i, 1].astype(F32)
            if i == 3:
                sown[0] = s0
                sown[1] = s1
                continue
            part[j, 0] = s0.astype(BF16)
            part[j, 1] = s1.astype(BF16)
            if i == 0:
                ra = remote(part.at[j, 0], relay_in.at[0], rl_s.at[0], rl_r.at[0], right)
                rb = remote(part.at[j, 1], relay_in.at[1], rl_s.at[1], rl_r.at[1], left)
                ra.start()
                rb.start()
            elif i == 1:
                d0 = remote(part.at[j, 1], rs_in.at[0], rs_s.at[0], rs_r.at[0], right)
                d0.start()
            else:
                d1 = remote(part.at[j, 0], rs_in.at[1], rs_s.at[1], rs_r.at[1], left)
                d1.start()
        jr = c * R + chip(1)
        jl = c * R + chip(3)
        ra.wait_recv()
        part[jr, 0] = (part[jr, 0].astype(F32) + relay_in[0].astype(F32)).astype(BF16)
        d2 = remote(part.at[jr, 0], rs_in.at[2], rs_s.at[2], rs_r.at[2], right)
        d2.start()
        rb.wait_recv()
        part[jl, 1] = (part[jl, 1].astype(F32) + relay_in[1].astype(F32)).astype(BF16)
        d3 = remote(part.at[jl, 1], rs_in.at[3], rs_s.at[3], rs_r.at[3], left)
        d3.start()
        d1.wait_recv()
        d0.wait_recv()
        own = c * NB + x * 2
        t0 = hbuf[own].astype(F32)
        t1 = hbuf[own + 1].astype(F32)
        s0 = sown[0] + rs_in[1].astype(F32)
        s1 = sown[1] + rs_in[0].astype(F32)
        d2.wait_recv()
        hbuf[own] = (t0 + (s0 + rs_in[2].astype(F32))).astype(BF16)
        d3.wait_recv()
        hbuf[own + 1] = (t1 + (s1 + rs_in[3].astype(F32))).astype(BF16)

        def piece(cc, b, h):
            return hbuf.at[cc * NB + b * 2 + h]

        lb, rb_, ob = chip(3), chip(1), chip(2)
        a0 = remote(piece(c, x, 0), piece(c, x, 0), ag_s.at[0], ag_r.at[0], right)
        a1 = remote(piece(c, x, 1), piece(c, x, 1), ag_s.at[1], ag_r.at[1], left)
        a2 = remote(piece(c, x, 1), piece(c, x, 1), ag_s.at[2], ag_r.at[2], right)
        a3 = remote(piece(c, x, 0), piece(c, x, 0), ag_s.at[3], ag_r.at[3], left)
        own2 = hbuf.at[pl.ds(own, 2)]
        p0 = remote(own2, own2, ad_s.at[0], ad_r.at[0], partner)
        for d in (a0, a1, a2, a3, p0):
            d.start()

        def fwd(k, ref):
            d = remote(ref, ref, ad_s.at[k], ad_r.at[k], partner)
            d.start()
            return d

        a0.wait_recv()
        a4 = remote(piece(c, lb, 0), piece(c, lb, 0), ag_s.at[4], ag_r.at[4], right)
        a4.start()
        f1 = fwd(1, piece(c, lb, 0))
        a1.wait_recv()
        a5 = remote(piece(c, rb_, 1), piece(c, rb_, 1), ag_s.at[5], ag_r.at[5], left)
        a5.start()
        f2 = fwd(2, piece(c, rb_, 1))
        a2.wait_recv()
        f3 = fwd(3, piece(c, lb, 1))
        a3.wait_recv()
        f4 = fwd(4, piece(c, rb_, 0))
        a4.wait_recv()
        f5 = fwd(5, piece(c, ob, 0))
        a5.wait_recv()
        f6 = fwd(6, piece(c, ob, 1))
        for d in (p0, f1, f2, f3, f4, f5, f6):
            d.wait_recv()
        for d in pair + [ra, rb, d0, d1, d2, d3, a0, a1, a2, a3, a4, a5, p0, f1, f2, f3, f4, f5, f6]:
            d.wait_send()

    def layer(l, carry):
        more = l + 1 < L

        norm(l, ga_ref)
        pool[...] = jnp.zeros_like(pool)

        def qkv_step(i, carry):
            b = ag_chip(i)
            for cc in range(2):
                cp_q(l, cc * R + b).wait()
            for n0, nw in tiles(NQ):
                accumulate(5 * grp + n0 // LW, group_dot(wq, b, n0, nw))
            return carry
        lax.fori_loop(0, R, qkv_step, 0)

        @pl.when(l == 0)
        def _():
            for j in blocks(AG_ORDER):
                cp_g(0, j).start()
                cp_u(0, j).start()
            for j in range(NB):
                cp_d(0, j).start()

        @pl.when(more)
        def _():
            for j in blocks(AG_ORDER):
                cp_q(l + 1, j).start()

        def rope(t):
            return (t * cosb[...] + pltpu.roll(t, hd // 2, 1) * sinb[...]).astype(BF16).astype(F32)

        def head(i):
            return pool[unit(5 * grp + i), :].astype(BF16).astype(F32)

        kn = rope(head(grp))
        vn = head(grp + 1)
        for g in range(grp):
            qrow[pl.ds(g, n, stride=grp), :] = rope(head(g))
            krow[pl.ds(g, n, stride=grp), :] = kn
            vrow[pl.ds(g, n, stride=grp), :] = vn

        first = lax.broadcasted_iota(jnp.int32, (2 * grp, S), 0) < grp

        def qk_step(i, carry):
            for s2 in range(SLOTS_PER_STEP):
                s = i * SLOTS_PER_STEP + s2
                cp_k(l, s).wait()
                for t in range(0, T, 2):
                    r0 = pl.multiple_of((s * T + t) * grp, 2 * grp)
                    q8 = qrow[pl.ds(r0, 2 * grp), :].astype(BF16)
                    k2 = kv[s, t:t + 2].reshape(2 * S, hd)
                    o = _dot_nt(q8, k2)
                    arow[pl.ds(r0, 2 * grp), :] = jnp.where(first, o[:, :S], o[:, S:])
            for s2 in range(SLOTS_PER_STEP):
                cp_v(l, i * SLOTS_PER_STEP + s2).start()
            return carry
        lax.fori_loop(0, SLOTS // SLOTS_PER_STEP, qk_step, 0)

        scale = hd ** -0.5
        CH = n * grp // 4
        for ch in range(4):
            rs = slice(ch * CH, (ch + 1) * CH)
            pos = lax.broadcasted_iota(jnp.int32, (CH, S), 1).astype(F32)
            sc = jnp.where(pos < lrow[rs, :], arow[rs, :] * scale, -jnp.inf)
            s_n = jnp.sum(qrow[rs, :] * krow[rs, :], axis=-1, keepdims=True) * scale
            m = jnp.maximum(jnp.max(sc, axis=-1, keepdims=True), s_n)
            p_c = jnp.exp(sc - m)
            p_n = jnp.exp(s_n - m)
            den = jnp.sum(p_c, axis=-1, keepdims=True) + p_n
            prow[rs, :] = p_c
            krow[rs, :] = jnp.broadcast_to(den, (CH, S))
            vrow[rs, :] = vrow[rs, :] * p_n

        def pv_step(i, carry):
            for s2 in range(SLOTS_PER_STEP):
                s = i * SLOTS_PER_STEP + s2
                cp_v(l, s).wait()
                for t in range(0, T, 2):
                    r0 = pl.multiple_of((s * T + t) * grp, 2 * grp)
                    p8 = prow[pl.ds(r0, 2 * grp), :]
                    pp = jnp.concatenate([jnp.where(first, p8, 0.0), jnp.where(first, 0.0, p8)], axis=1).astype(BF16)
                    o = _dot(pp, kv[s, t:t + 2].reshape(2 * S, hd))
                    arow[pl.ds(r0, 2 * grp), :] = o

            @pl.when(more)
            def _():
                for s2 in range(SLOTS_PER_STEP):
                    cp_k(l + 1, i * SLOTS_PER_STEP + s2).start()
            return carry
        lax.fori_loop(0, SLOTS // SLOTS_PER_STEP, pv_step, 0)

        for ch in range(4):
            rs = slice(ch * CH, (ch + 1) * CH)
            arow[rs, :] = (arow[rs, :] + vrow[rs, :]) / krow[rs, :]
        for g in range(grp):
            att[:, g * hd:(g + 1) * hd] = arow[pl.ds(g, n, stride=grp), :].astype(BF16)

        @pl.when(l == 0)
        def _():
            pl.semaphore_wait(barrier, 3)

        all_reduce(lambda j: _dot(att[...], wo[:, cols(j * BW, BW)]), lambda j: cp_o(l, j).wait())

        @pl.when(more)
        def _():
            for j in range(NB):
                cp_o(l + 1, j).start()

        norm(l, gm_ref)
        pool[...] = jnp.zeros_like(pool)

        def mlp_step(i, carry):
            b = ag_chip(i)
            for cc in range(2):
                cp_g(l, cc * R + b).wait()
                cp_u(l, cc * R + b).wait()
            for k, w in enumerate((wg, wu)):
                for n0, nw in tiles(F):
                    accumulate((k * F + n0) // LW, group_dot(w, b, n0, nw))
            return carry
        lax.fori_loop(0, R, mlp_step, 0)

        @pl.when(more)
        def _():
            for j in blocks(AG_ORDER):
                cp_g(l + 1, j).start()
                cp_u(l + 1, j).start()

        for u in range(F // LW):
            act[:, u * LW:(u + 1) * LW] = (jax.nn.silu(pool[unit(u), :]) * pool[unit(F // LW + u), :]).astype(BF16)

        all_reduce(lambda j: _dot(act[...], wd[:, cols(j * BW, BW)]), lambda j: cp_d(l, j).wait())

        @pl.when(more)
        def _():
            for j in range(NB):
                cp_d(l + 1, j).start()
        return carry

    lax.fori_loop(0, L, layer, 0)

    outs = [pltpu.make_async_copy(hbuf.at[p], y_hbm.at[:, cols(p * PW, PW)], s_y.at[p]) for p in range(2 * NB)]
    for d in outs:
        d.start()
    for d in outs:
        d.wait()


def solution(mesh):
    tp = mesh.shape["tp"]

    def body(x, g_attn, w_qkv, w_o, g_mlp, w_gate, w_up, w_down, k_cache, v_cache, lengths):
        n, D = x.shape
        L, _, NQ = w_qkv.shape
        KO, F = w_o.shape[1], w_gate.shape[2]
        S, hd = k_cache.shape[2], k_cache.shape[4]
        R = tp // 2
        NB, PW, BW = tp, D // tp // 2, D // tp
        grp = KO // hd
        kc = k_cache.reshape(L, n, S, hd)
        vc = v_cache.reshape(L, n, S, hd)
        half = hd // 2
        inv = np.float32(ROPE_THETA) ** (-np.arange(half, dtype=np.float32) * np.float32(2.0) / np.float32(hd))
        inv = jnp.asarray(np.concatenate([inv, inv])[None, :].astype(np.float32))
        dims = (L, n, D, NQ, KO, F, S, hd, R)
        anyspec = pl.BlockSpec(memory_space=pl.ANY)
        vspec = pl.BlockSpec(memory_space=pltpu.VMEM)
        V = pltpu.VMEM
        DMA = pltpu.SemaphoreType.DMA
        rows = n * grp
        scratch = [
            V((D, NQ), BF16), V((KO, D), BF16), V((D, F), BF16), V((D, F), BF16), V((F, D), BF16),
            V((SLOTS, n // SLOTS, S, hd), BF16),
            V((2 * NB, n, PW), BF16), V((2 * NB, n, PW), BF16),
            V((NB, 2, n, PW), BF16), V((R, 2, n, PW), BF16), V((2, n, PW), BF16), V((4, n, PW), BF16), V((2, n, PW), F32),
            V((max(2 * F // 128, 5 * grp + NQ // 128) * n, 128), F32), V((n, F), BF16),
            V((rows, hd), F32), V((n, hd), F32), V((n, hd), F32), V((n, KO), BF16),
            DMA((2 * NB,)), DMA((NB,)), DMA((NB,)), DMA((NB,)), DMA((NB,)), DMA((NB,)), DMA((SLOTS,)), DMA((2 * NB,)),
            DMA((4,)), DMA((4,)), DMA((2,)), DMA((2,)), DMA((4,)), DMA((4,)), DMA((6,)), DMA((6,)), DMA((7,)), DMA((7,)),
        ]
        return pl.pallas_call(
            functools.partial(_kernel, dims),
            out_shape=jax.ShapeDtypeStruct((n, D), BF16),
            in_specs=[anyspec, vspec, anyspec, anyspec, vspec, anyspec, anyspec, anyspec, anyspec, anyspec, vspec, vspec],
            out_specs=anyspec,
            scratch_shapes=scratch,
            compiler_params=pltpu.CompilerParams(collective_id=0, has_side_effects=True, vmem_limit_bytes=67043328),
        )(x, g_attn, w_qkv, w_o, g_mlp, w_gate, w_up, w_down, kc, vc, lengths.reshape(1, n), inv)

    col = P(None, None, 'tp')
    row = P(None, 'tp', None)
    cache = P(None, 'dp', None, 'tp', None)
    return jax.shard_map(body, mesh=mesh,
                         in_specs=(P('dp', None), P(), col, row, P(), col, col, row, cache, cache, P('dp')),
                         out_specs=P('dp', None), check_vma=False)
```

```python
import functools

import jax
import jax.numpy as jnp
import numpy as np
from jax import lax
from jax.experimental import pallas as pl
from jax.experimental.pallas import tpu as pltpu
from jax.sharding import PartitionSpec as P

EPS = 1e-5
ROPE_THETA = 500000.0
F32 = jnp.float32
BF16 = jnp.bfloat16
SLOTS = 8
SLOTS_PER_STEP = 2
RS_ORDER = (2, 1, 3, 0)


def _dot(a, b):
    return jnp.dot(a, b, preferred_element_type=F32)


def _dot_nt(a, b):
    return lax.dot_general(a, b, (((1,), (1,)), ((), ())), preferred_element_type=F32)


def _kernel(dims, x_hbm, ga_ref, wqkv_hbm, wo_hbm, gm_ref, wg_hbm, wu_hbm, wd_hbm, kc_hbm, vc_hbm, len_ref, inv_ref,
            y_hbm,
            wq, wo, wg, wu, wd, kv, hbuf, abuf, part, pair_in, relay_in, rs_in, sown, pool, act, lrow, cosb, sinb, att, rbuf, stat,
            s_x, s_q, s_o, s_g, s_u, s_d, s_kv, s_y,
            pr_s, pr_r, rl_s, rl_r, rs_s, rs_r, ag_s, ag_r, ad_s, ad_r, st_s, st_r):
    L, n, D, NQ, KO, F, S, hd, R = dims
    NB = 2 * R
    BW = D // NB
    PW = BW // 2
    grp = KO // hd
    T = n // SLOTS
    LW = 128
    NR = n * grp
    qrow, krow, vrow, arow, prow = (pool.at[pl.ds(i * NR, NR)] for i in range(5))
    tp = lax.axis_index("tp")
    x = tp // 2
    c = tp % 2
    right = {"tp": ((x + 1) % R) * 2 + c}
    left = {"tp": ((x + R - 1) % R) * 2 + c}
    partner = {"tp": x * 2 + (1 - c)}
    MESH = pl.DeviceIdType.MESH

    def chip(off):
        return (x + off) % R

    def cols(start, size):
        return pl.ds(pl.multiple_of(start, 128), size)

    def rows(start, size):
        return pl.ds(pl.multiple_of(start, 128), size)

    def cp_x(p):
        return pltpu.make_async_copy(x_hbm.at[:, cols(p * PW, PW)], hbuf.at[p], s_x.at[p])

    def cp_q(l, j):
        return pltpu.make_async_copy(wqkv_hbm.at[l, rows(j * BW, BW), :], wq.at[rows(j * BW, BW), :], s_q.at[j])

    def cp_o(l, j):
        return pltpu.make_async_copy(wo_hbm.at[l, :, cols(j * BW, BW)], wo.at[:, cols(j * BW, BW)], s_o.at[j])

    def cp_g(l, j):
        return pltpu.make_async_copy(wg_hbm.at[l, rows(j * BW, BW), :], wg.at[rows(j * BW, BW), :], s_g.at[j])

    def cp_u(l, j):
        return pltpu.make_async_copy(wu_hbm.at[l, rows(j * BW, BW), :], wu.at[rows(j * BW, BW), :], s_u.at[j])

    def cp_d(l, j):
        return pltpu.make_async_copy(wd_hbm.at[l, :, cols(j * BW, BW)], wd.at[:, cols(j * BW, BW)], s_d.at[j])

    def cp_k(l, s):
        return pltpu.make_async_copy(kc_hbm.at[l, pl.ds(s * T, T)], kv.at[s], s_kv.at[s])

    def cp_v(l, s):
        return pltpu.make_async_copy(vc_hbm.at[l, pl.ds(s * T, T)], kv.at[s], s_kv.at[s])

    scope = jax.named_scope
    barrier = pltpu.get_barrier_semaphore()
    peers = [{"tp": (tp + k) % NB} for k in range(1, NB)]
    for d in peers:
        pl.semaphore_signal(barrier, inc=1, device_id=d, device_id_type=MESH)

    lb, rb, ob = chip(3), chip(1), chip(2)
    GROUPS = ((c * R + x, (1 - c) * R + x), (c * R + lb, c * R + rb), ((1 - c) * R + lb, (1 - c) * R + rb),
              (c * R + ob, (1 - c) * R + ob))
    NG = len(GROUPS)
    blocks = [j for g in GROUPS for j in g]

    for p in range(2 * NB):
        cp_x(p).start()

    lcol = jnp.broadcast_to(len_ref[...].astype(F32), (hd, n)).T
    ang = lcol * inv_ref[...]
    lane = lax.broadcasted_iota(jnp.int32, (n, hd), 1)
    for j in blocks:
        cp_q(0, j).start()
    cosb[...] = jnp.cos(ang)
    sn = jnp.sin(ang)
    sinb[...] = jnp.where(lane < hd // 2, -sn, sn)
    for g in range(grp):
        lrow[pl.ds(g, n, stride=grp), :] = lcol

    def remote(src, dst, ss, rs, dev):
        return pltpu.make_async_remote_copy(src_ref=src, dst_ref=dst, send_sem=ss, recv_sem=rs, device_id=dev,
                                            device_id_type=MESH)

    def halves(width):
        return [(k, k + LW) for k in range(0, width, LW)]

    def put_scale(row):
        rbuf[...] = jnp.broadcast_to(row, (LW, n)).T

    def local_scale():
        def sq(p, s):
            v = hbuf[p].astype(F32)
            return s + v * v
        s = lax.fori_loop(0, 2 * NB, sq, jnp.zeros((n, PW), F32))
        r = lax.rsqrt(jnp.sum(s, axis=-1, keepdims=True) * (1.0 / D) + EPS)
        rbuf[...] = jnp.broadcast_to(r, (n, LW))

    def normalize(l, ref, j):
        for h in range(2):
            p = j * 2 + h
            for a, b in halves(PW):
                g = ref[l:l + 1, cols(p * PW + a, LW)].astype(F32)
                abuf[p, :, a:b] = (hbuf[p, :, a:b].astype(F32) * rbuf[...] * g).astype(BF16)

    def group_dot(w, js, n0, nw):
        s = None
        for j in js:
            for h in range(2):
                d = _dot(abuf[j * 2 + h], w[rows(j * BW + h * PW, PW), n0:n0 + nw])
                s = d if s is None else s + d
        return s

    def unit(i):
        return pl.ds(i * n, n)

    def tiles(width):
        return [(n0, min(256, width - n0)) for n0 in range(0, width, 256)]

    def accumulate(u, d, first):
        for k, (a, b) in enumerate(halves(d.shape[1])):
            if first:
                pool[unit(u + k), :] = d[:, a:b]
            else:
                pool[unit(u + k), :] += d[:, a:b]

    UH = n // 2

    def half_rows(u):
        return pl.ds(u * UH, UH)

    def reduce_scatter(block, wait_w, early):
        pair = []

        def other(i):
            j = (1 - c) * R + chip(RS_ORDER[i])
            wait_w(j)
            o = block(j).astype(BF16)
            part[j, 0] = o[:, :PW]
            part[j, 1] = o[:, PW:]
            d = remote(part.at[j], pair_in.at[i], pr_s.at[i], pr_r.at[i], partner)
            d.start()
            pair.append(d)

        def mine(i):
            j = c * R + chip(RS_ORDER[i])
            wait_w(j)
            o = block(j).astype(BF16)
            part[j, 0] = o[:, :PW]
            part[j, 1] = o[:, PW:]

        jo, jr, jl, jx = (c * R + chip(o) for o in RS_ORDER)
        work = [(other, 0), (other, 1), (mine, 0), (other, 2), (mine, 1), (other, 3), (mine, 2), (mine, 3)]
        with scope("rs_mm1"):
            for f, i in work[:early]:
                f(i)
        with scope("rs_wait1"):
            pair[0].wait_recv()
            m1 = []
            for h, dev in ((0, right), (1, left)):
                part[jo, h] = (part[jo, h].astype(F32) + pair_in[0, h].astype(F32)).astype(BF16)
                for u in range(2):
                    d = remote(part.at[jo, h, half_rows(u)], relay_in.at[h, half_rows(u)], rl_s.at[h * 2 + u],
                               rl_r.at[h * 2 + u], dev)
                    d.start()
                    m1.append(d)
        with scope("rs_mm2"):
            for f, i in work[early:]:
                f(i)
        with scope("rs_wait2"):
            for i, j in ((1, jr), (2, jl)):
                pair[i].wait_recv()
                for h in range(2):
                    part[j, h] = (part[j, h].astype(F32) + pair_in[i, h].astype(F32)).astype(BF16)
        with scope("rs_send2"):
            for d in m1:
                d.wait_send()
            m2 = [remote(part.at[jr, 1], rs_in.at[0], rs_s.at[0], rs_r.at[0], right),
                  remote(part.at[jl, 0], rs_in.at[1], rs_s.at[1], rs_r.at[1], left)]
            for d in m2:
                d.start()
            pair[3].wait_recv()
            for h in range(2):
                sown[h] = part[jx, h].astype(F32) + pair_in[3, h].astype(F32)
        with scope("rs_relay"):
            m3 = []
            for u in range(2):
                for h, j, dev in ((0, jr, right), (1, jl, left)):
                    m1[h * 2 + u].wait_recv()
                    ru = half_rows(u)
                    part[j, h, ru] = (part[j, h, ru].astype(F32) + relay_in[h, ru].astype(F32)).astype(BF16)
                    d = remote(part.at[j, h, ru], rs_in.at[2 + h, ru], rs_s.at[2 + h * 2 + u], rs_r.at[2 + h * 2 + u], dev)
                    d.start()
                    m3.append((h, u, d))
        own = (c * R + x) * 2
        with scope("rs_sum"):
            for h in range(2):
                m2[1 - h].wait_recv()
                sown[h] = sown[h] + rs_in[1 - h].astype(F32)
        with scope("rs_fin"):
            first = [None] * 4
            for h, u, d in m3:
                d.wait_recv()
                ru = half_rows(u)
                hbuf[own + h, ru] = (hbuf[own + h, ru].astype(F32) + (sown[h, ru] + rs_in[2 + h, ru].astype(F32))).astype(BF16)
                ref = hbuf.at[own + h, ru]
                a = remote(ref, ref, ag_s.at[h * 2 + u], ag_r.at[h * 2 + u], (right, left)[h])
                a.start()
                first[h * 2 + u] = a
        done = [d for d in pair] + m2 + [d for _, _, d in m3]
        return first, done

    def gather(first, done, stats, use):
        own = (c * R + x) * 2
        own2 = hbuf.at[pl.ds(own, 2)]
        p0 = remote(own2, own2, ad_s.at[0], ad_r.at[0], partner)
        p0.start()
        done = done + [p0]
        st = []
        with scope("stats"):
            if stats:
                q = None
                for h in range(2):
                    for a, b in halves(PW):
                        v = hbuf[own + h, :, a:b].astype(F32)
                        q = v * v if q is None else q + v * v
                sq = jnp.broadcast_to(jnp.sum(q.T, axis=0, keepdims=True), (8, n))
                stat[0] = sq
                for k in (4, 3, 5, 2, 6, 1, 7):
                    d = remote(stat.at[0], stat.at[k], st_s.at[k - 1], st_r.at[k - 1], peers[k - 1])
                    d.start()
                    st.append(d)
        with scope("ag_send2"):
            for d in first:
                d.wait_send()

            def piece(b, h):
                return hbuf.at[(c * R + b) * 2 + h]
            second = [remote(piece(x, 1), piece(x, 1), ag_s.at[4], ag_r.at[4], right),
                      remote(piece(x, 0), piece(x, 0), ag_s.at[5], ag_r.at[5], left)]
            for d in second:
                d.start()

        fw = []

        def forward(k, ref):
            d = remote(ref, ref, ad_s.at[k], ad_r.at[k], partner)
            d.start()
            fw.append(d)

        relay = []
        with scope("ag_relay"):
            for u in range(2):
                for h, b, dev in ((0, lb, right), (1, rb, left)):
                    first[h * 2 + u].wait_recv()
                    ref = hbuf.at[(c * R + b) * 2 + h, half_rows(u)]
                    d = remote(ref, ref, ag_s.at[6 + h * 2 + u], ag_r.at[6 + h * 2 + u], dev)
                    d.start()
                    relay.append(d)
                    forward(1 + h * 2 + u, ref)
        with scope("ag_stats"):
            if stats:
                for d in st:
                    d.wait_recv()
                t = stat[0]
                for k in range(1, NB):
                    t = t + stat[k]
                put_scale(lax.rsqrt(t[0:1] * (1.0 / D) + EPS))
        with scope("use0"):
            p0.wait_recv()
            use(0)
        with scope("ag_2"):
            second[0].wait_recv()
            forward(5, piece(lb, 1))
            second[1].wait_recv()
            forward(6, piece(rb, 0))
        with scope("use1"):
            use(1)
        with scope("ag_3"):
            for u in range(2):
                for h in range(2):
                    relay[u * 2 + h].wait_recv()
                    forward(7 + h * 2 + u, hbuf.at[(c * R + ob) * 2 + h, half_rows(u)])
        with scope("ag_fw1"):
            for d in fw[:6]:
                d.wait_recv()
        with scope("use2"):
            use(2)
        with scope("ag_fw2"):
            for d in fw[6:]:
                d.wait_recv()
        with scope("use3"):
            use(3)
        with scope("ag_drain"):
            for d in done + second + relay + fw + st:
                d.wait_send()

    def qkv_use(l):
        def use(g):
            js = GROUPS[g]
            for j in js:
                normalize(l, ga_ref, j)
            for j in js:
                cp_q(l, j).wait()
            for n0, nw in tiles(NQ):
                accumulate(5 * grp + n0 // LW, group_dot(wq, js, n0, nw), g == 0)
        return use

    first_row = lax.broadcasted_iota(jnp.int32, (2 * grp, S), 0) < grp
    scale = hd ** -0.5
    CH = NR // 4

    def attention(l):
        def rope(t):
            return (t * cosb[...] + pltpu.roll(t, hd // 2, 1) * sinb[...]).astype(BF16).astype(F32)

        def head(i):
            return pool[unit(5 * grp + i), :].astype(BF16).astype(F32)

        with scope("rope"):
            kn = rope(head(grp))
            vn = head(grp + 1)
            for g in range(grp):
                qrow[pl.ds(g, n, stride=grp), :] = rope(head(g))
                krow[pl.ds(g, n, stride=grp), :] = kn
                vrow[pl.ds(g, n, stride=grp), :] = vn

        def qk_step(i, carry):
            for s2 in range(SLOTS_PER_STEP):
                s = i * SLOTS_PER_STEP + s2
                cp_k(l, s).wait()
                for t in range(0, T, 2):
                    r0 = pl.multiple_of((s * T + t) * grp, 2 * grp)
                    q8 = qrow[pl.ds(r0, 2 * grp), :].astype(BF16)
                    o = _dot_nt(q8, kv[s, t:t + 2].reshape(2 * S, hd))
                    arow[pl.ds(r0, 2 * grp), :] = jnp.where(first_row, o[:, :S], o[:, S:])
            for s2 in range(SLOTS_PER_STEP):
                cp_v(l, i * SLOTS_PER_STEP + s2).start()
            return carry
        with scope("qk"):
            lax.fori_loop(0, SLOTS // SLOTS_PER_STEP, qk_step, 0)

        with scope("softmax"):
            for ch in range(4):
                rs = slice(ch * CH, (ch + 1) * CH)
                pos = lax.broadcasted_iota(jnp.int32, (CH, S), 1).astype(F32)
                sc = jnp.where(pos < lrow[rs, :], arow[rs, :] * scale, -jnp.inf)
                s_n = jnp.sum(qrow[rs, :] * krow[rs, :], axis=-1, keepdims=True) * scale
                m = jnp.maximum(jnp.max(sc, axis=-1, keepdims=True), s_n)
                p_c = jnp.exp(sc - m)
                p_n = jnp.exp(s_n - m)
                den = jnp.sum(p_c, axis=-1, keepdims=True) + p_n
                prow[rs, :] = p_c
                krow[rs, :] = jnp.broadcast_to(den, (CH, S))
                vrow[rs, :] = vrow[rs, :] * p_n

        def pv_step(i, carry):
            for s2 in range(SLOTS_PER_STEP):
                s = i * SLOTS_PER_STEP + s2
                cp_v(l, s).wait()
                for t in range(0, T, 2):
                    r0 = pl.multiple_of((s * T + t) * grp, 2 * grp)
                    p8 = prow[pl.ds(r0, 2 * grp), :]
                    pp = jnp.concatenate([jnp.where(first_row, p8, 0.0), jnp.where(first_row, 0.0, p8)], axis=1).astype(BF16)
                    arow[pl.ds(r0, 2 * grp), :] = _dot(pp, kv[s, t:t + 2].reshape(2 * S, hd))
            return carry
        with scope("pv"):
            lax.fori_loop(0, SLOTS // SLOTS_PER_STEP, pv_step, 0)

        with scope("att_out"):
            for ch in range(4):
                rs = slice(ch * CH, (ch + 1) * CH)
                arow[rs, :] = (arow[rs, :] + vrow[rs, :]) / krow[rs, :]
            for g in range(grp):
                att[:, g * hd:(g + 1) * hd] = arow[pl.ds(g, n, stride=grp), :].astype(BF16)

    def mlp_use(l):
        FU = F // LW

        def use(g):
            js = GROUPS[g]
            for j in js:
                normalize(l, gm_ref, j)
            for j in js:
                cp_g(l, j).wait()
                cp_u(l, j).wait()
            for n0, nw in tiles(F):
                if g < NG - 1:
                    for k, w in enumerate((wg, wu)):
                        accumulate((k * F + n0) // LW, group_dot(w, js, n0, nw), g == 0)
                else:
                    dg, du = group_dot(wg, js, n0, nw), group_dot(wu, js, n0, nw)
                    for k, (a, b) in enumerate(halves(nw)):
                        u = n0 // LW + k
                        gate = pool[unit(u), :] + dg[:, a:b]
                        up = pool[unit(FU + u), :] + du[:, a:b]
                        act[:, n0 + a:n0 + b] = (jax.nn.silu(gate) * up).astype(BF16)
        return use

    with scope("x_wait"):
        for p in range(2 * NB):
            cp_x(p).wait()
    with scope("scale0"):
        for s in range(SLOTS):
            cp_k(0, s).start()
        for j in range(NB):
            cp_o(0, j).start()
        local_scale()

    outs = []

    def out_use(g):
        for j in GROUPS[g]:
            for h in range(2):
                p = j * 2 + h
                d = pltpu.make_async_copy(hbuf.at[p], y_hbm.at[:, cols(p * PW, PW)], s_y.at[g * 4 + len(outs) % 4])
                d.start()
                outs.append(d)

    pending = None
    for l in range(L):
        if pending is None:
            for g in range(NG):
                with scope("qkv"):
                    qkv_use(l)(g)
        else:
            gather(*pending, True, qkv_use(l))
        attention(l)
        if l == 0:
            for j in blocks:
                cp_g(0, j).start()
                cp_u(0, j).start()
            for j in range(NB):
                cp_d(0, j).start()
            pl.semaphore_wait(barrier, NB - 1)
        pending = reduce_scatter(lambda j: _dot(att[...], wo[:, cols(j * BW, BW)]), lambda j: cp_o(l, j).wait(), 8)
        if l + 1 < L:
            for j in range(NB):
                cp_o(l + 1, j).start()
        gather(*pending, True, mlp_use(l))
        if l + 1 < L:
            for j in blocks:
                cp_q(l + 1, j).start()
            for s in range(SLOTS):
                cp_k(l + 1, s).start()
            for j in blocks:
                cp_g(l + 1, j).start()
                cp_u(l + 1, j).start()
        pending = reduce_scatter(lambda j: _dot(act[...], wd[:, cols(j * BW, BW)]), lambda j: cp_d(l, j).wait(), 3)
        if l + 1 < L:
            for j in range(NB):
                cp_d(l + 1, j).start()
    gather(*pending, False, out_use)
    with scope("y_out"):
        for d in outs:
            d.wait()


def solution(mesh):
    tp = mesh.shape["tp"]

    def body(x, g_attn, w_qkv, w_o, g_mlp, w_gate, w_up, w_down, k_cache, v_cache, lengths):
        n, D = x.shape
        L, _, NQ = w_qkv.shape
        KO, F = w_o.shape[1], w_gate.shape[2]
        S, hd = k_cache.shape[2], k_cache.shape[4]
        R = tp // 2
        NB, PW, BW = tp, D // tp // 2, D // tp
        grp = KO // hd
        kc = k_cache.reshape(L, n, S, hd)
        vc = v_cache.reshape(L, n, S, hd)
        half = hd // 2
        inv = np.float32(ROPE_THETA) ** (-np.arange(half, dtype=np.float32) * np.float32(2.0) / np.float32(hd))
        inv = jnp.asarray(np.concatenate([inv, inv])[None, :].astype(np.float32))
        dims = (L, n, D, NQ, KO, F, S, hd, R)
        anyspec = pl.BlockSpec(memory_space=pl.ANY)
        vspec = pl.BlockSpec(memory_space=pltpu.VMEM)
        V = pltpu.VMEM
        DMA = pltpu.SemaphoreType.DMA
        rows = n * grp
        scratch = [
            V((D, NQ), BF16), V((KO, D), BF16), V((D, F), BF16), V((D, F), BF16), V((F, D), BF16),
            V((SLOTS, n // SLOTS, S, hd), BF16),
            V((2 * NB, n, PW), BF16), V((2 * NB, n, PW), BF16),
            V((NB, 2, n, PW), BF16), V((R, 2, n, PW), BF16), V((2, n, PW), BF16), V((4, n, PW), BF16), V((2, n, PW), F32),
            V((max(2 * F // 128, 5 * grp + NQ // 128) * n, 128), F32), V((n, F), BF16),
            V((rows, hd), F32), V((n, hd), F32), V((n, hd), F32), V((n, KO), BF16), V((n, 128), F32), V((NB, 8, n), F32),
            DMA((2 * NB,)), DMA((NB,)), DMA((NB,)), DMA((NB,)), DMA((NB,)), DMA((NB,)), DMA((SLOTS,)), DMA((2 * NB,)),
            DMA((4,)), DMA((4,)), DMA((4,)), DMA((4,)), DMA((6,)), DMA((6,)), DMA((10,)), DMA((10,)), DMA((11,)), DMA((11,)),
            DMA((NB - 1,)), DMA((NB - 1,)),
        ]
        return pl.pallas_call(
            functools.partial(_kernel, dims),
            out_shape=jax.ShapeDtypeStruct((n, D), BF16),
            in_specs=[anyspec, vspec, anyspec, anyspec, vspec, anyspec, anyspec, anyspec, anyspec, anyspec, vspec, vspec],
            out_specs=anyspec,
            scratch_shapes=scratch,
            compiler_params=pltpu.CompilerParams(collective_id=0, has_side_effects=True, vmem_limit_bytes=67043328),
        )(x, g_attn, w_qkv, w_o, g_mlp, w_gate, w_up, w_down, kc, vc, lengths.reshape(1, n), inv)

    col = P(None, None, 'tp')
    row = P(None, 'tp', None)
    cache = P(None, 'dp', None, 'tp', None)
    return jax.shard_map(body, mesh=mesh,
                         in_specs=(P('dp', None), P(), col, row, P(), col, col, row, cache, cache, P('dp')),
                         out_specs=P('dp', None), check_vma=False)
```

```python
import functools

import jax
import jax.numpy as jnp
import numpy as np
from jax import lax
from jax.experimental import pallas as pl
from jax.experimental.pallas import tpu as pltpu
from jax.sharding import PartitionSpec as P

EPS = 1e-5
ROPE_THETA = 500000.0
F32 = jnp.float32
BF16 = jnp.bfloat16
SLOTS = 8
SLOTS_PER_STEP = 4
U = 4
RS_ORDER = (2, 1, 3, 0)


def _dot(a, b):
    return jnp.dot(a, b, preferred_element_type=F32)


def _dot_nt(a, b):
    return lax.dot_general(a, b, (((1,), (1,)), ((), ())), preferred_element_type=F32)


def _kernel(dims, x_hbm, ga_hbm, wqkv_hbm, wo_hbm, gm_hbm, wg_hbm, wu_hbm, wd_hbm, kc_hbm, vc_hbm, len_hbm, inv_hbm,
            y_hbm,
            wq, wo, wg, wu, wd, kv, hbuf, abuf, part, pair_in, relay_in, rs_in, sown, pool, act, lrow, cosb, sinb, att, rbuf, stat, ga_ref, gm_ref, len_ref, inv_ref, s_c,
            s_x, s_q, s_o, s_g, s_u, s_d, s_kv, s_y,
            pr_s, pr_r, rl_s, rl_r, rs_s, rs_r, ag_s, ag_r, ad_s, ad_r, st_s, st_r):
    L, n, D, NQ, KO, F, S, hd, R = dims
    NB = 2 * R
    BW = D // NB
    PW = BW // 2
    grp = KO // hd
    T = n // SLOTS
    LW = 128
    NR = n * grp
    qrow, krow, vrow, arow, prow = (pool.at[pl.ds(i * NR, NR)] for i in range(5))
    tp = lax.axis_index("tp")
    x = tp // 2
    c = tp % 2
    right = {"tp": ((x + 1) % R) * 2 + c}
    left = {"tp": ((x + R - 1) % R) * 2 + c}
    partner = {"tp": x * 2 + (1 - c)}
    MESH = pl.DeviceIdType.MESH

    def chip(off):
        return (x + off) % R

    def cols(start, size):
        return pl.ds(pl.multiple_of(start, 128), size)

    def rows(start, size):
        return pl.ds(pl.multiple_of(start, 128), size)

    def cp_x(p):
        return pltpu.make_async_copy(x_hbm.at[:, cols(p * PW, PW)], hbuf.at[p], s_x.at[p])

    def cp_q(l, j):
        return pltpu.make_async_copy(wqkv_hbm.at[l, rows(j * BW, BW), :], wq.at[rows(j * BW, BW), :], s_q.at[j])

    def cp_o(l, j):
        return pltpu.make_async_copy(wo_hbm.at[l, :, cols(j * BW, BW)], wo.at[:, cols(j * BW, BW)], s_o.at[j])

    def cp_g(l, j):
        return pltpu.make_async_copy(wg_hbm.at[l, rows(j * BW, BW), :], wg.at[rows(j * BW, BW), :], s_g.at[j])

    def cp_u(l, j):
        return pltpu.make_async_copy(wu_hbm.at[l, rows(j * BW, BW), :], wu.at[rows(j * BW, BW), :], s_u.at[j])

    def cp_d(l, j):
        return pltpu.make_async_copy(wd_hbm.at[l, :, cols(j * BW, BW)], wd.at[:, cols(j * BW, BW)], s_d.at[j])

    def cp_k(l, s):
        return pltpu.make_async_copy(kc_hbm.at[l, pl.ds(s * T, T)], kv.at[s], s_kv.at[s])

    def cp_v(l, s):
        return pltpu.make_async_copy(vc_hbm.at[l, pl.ds(s * T, T)], kv.at[s], s_kv.at[s])

    scope = jax.named_scope
    barrier = pltpu.get_barrier_semaphore()
    peers = [{"tp": (tp + k) % NB} for k in range(1, NB)]

    lb, rb, ob = chip(3), chip(1), chip(2)
    GROUPS = ((c * R + x, (1 - c) * R + x), (c * R + lb, c * R + rb), ((1 - c) * R + lb, (1 - c) * R + rb),
              (c * R + ob, (1 - c) * R + ob))
    NG = len(GROUPS)
    blocks = [j for g in GROUPS for j in g]

    for p in range(2 * NB):
        cp_x(p).start()
    small = [pltpu.make_async_copy(a, b, s_c.at[i])
             for i, (a, b) in enumerate(((len_hbm, len_ref), (inv_hbm, inv_ref), (ga_hbm, ga_ref), (gm_hbm, gm_ref)))]
    for d in small:
        d.start()
    for j in blocks[:2]:
        cp_q(0, j).start()
    for d in peers:
        pl.semaphore_signal(barrier, inc=1, device_id=d, device_id_type=MESH)

    def tables():
        lcol = jnp.broadcast_to(len_ref[...].astype(F32), (hd, n)).T
        ang = lcol * inv_ref[...]
        lane = lax.broadcasted_iota(jnp.int32, (n, hd), 1)
        cosb[...] = jnp.cos(ang)
        sn = jnp.sin(ang)
        sinb[...] = jnp.where(lane < hd // 2, -sn, sn)
        for g in range(grp):
            lrow[pl.ds(g, n, stride=grp), :] = lcol

    def remote(src, dst, ss, rs, dev):
        return pltpu.make_async_remote_copy(src_ref=src, dst_ref=dst, send_sem=ss, recv_sem=rs, device_id=dev,
                                            device_id_type=MESH)

    def halves(width):
        return [(k, k + LW) for k in range(0, width, LW)]

    def put_scale(row):
        rbuf[...] = jnp.broadcast_to(row, (LW, n)).T

    def local_scale():
        def sq(p, s):
            v = hbuf[p].astype(F32)
            return s + v * v
        s = lax.fori_loop(0, 2 * NB, sq, jnp.zeros((n, PW), F32))
        r = lax.rsqrt(jnp.sum(s, axis=-1, keepdims=True) * (1.0 / D) + EPS)
        rbuf[...] = jnp.broadcast_to(r, (n, LW))

    def normalize(l, ref, j):
        for h in range(2):
            p = j * 2 + h
            for a, b in halves(PW):
                g = ref[l:l + 1, cols(p * PW + a, LW)].astype(F32)
                abuf[p, :, a:b] = (hbuf[p, :, a:b].astype(F32) * rbuf[...] * g).astype(BF16)

    def group_dot(w, js, n0, nw):
        s = None
        for j in js:
            for h in range(2):
                d = _dot(abuf[j * 2 + h], w[rows(j * BW + h * PW, PW), n0:n0 + nw])
                s = d if s is None else s + d
        return s

    def unit(i):
        return pl.ds(i * n, n)

    def tiles(width):
        return [(n0, min(256, width - n0)) for n0 in range(0, width, 256)]

    def accumulate(u, d, first):
        for k, (a, b) in enumerate(halves(d.shape[1])):
            if first:
                pool[unit(u + k), :] = d[:, a:b]
            else:
                pool[unit(u + k), :] += d[:, a:b]

    UH = n // U
    slow = jnp.where(x == 0, 1, 0)
    SIDES = (slow, 1 - slow)
    right_i, left_i = right["tp"], left["tp"]

    def side_dev(h):
        return {"tp": jnp.where(h == 0, right_i, left_i)}

    def half_rows(u):
        return pl.ds(u * UH, UH)

    def reduce_scatter(block, wait_w, early, then):
        pair = []

        def other(i):
            j = (1 - c) * R + chip(RS_ORDER[i])
            o = block(j).astype(BF16)
            part[j, 0] = o[:, :PW]
            part[j, 1] = o[:, PW:]
            d = remote(part.at[j], pair_in.at[i], pr_s.at[i], pr_r.at[i], partner)
            d.start()
            pair.append(d)

        def mine(i):
            j = c * R + chip(RS_ORDER[i])
            o = block(j).astype(BF16)
            part[j, 0] = o[:, :PW]
            part[j, 1] = o[:, PW:]

        jo, jr, jl, jx = (c * R + chip(o) for o in RS_ORDER)
        m1 = [remote(part.at[jo, h, half_rows(u)], relay_in.at[h, half_rows(u)], rl_s.at[h * U + u],
                     rl_r.at[h * U + u], (right, left)[h]) for h in range(2) for u in range(U)]
        m2 = [remote(part.at[jr, 1], rs_in.at[0], rs_s.at[0], rs_r.at[0], right),
              remote(part.at[jl, 0], rs_in.at[1], rs_s.at[1], rs_r.at[1], left)]

        def opposite(k):
            for u in range(k * U // 2, (k + 1) * U // 2):
                for h in range(2):
                    ru = half_rows(u)
                    part[jo, h, ru] = (part[jo, h, ru].astype(F32) + pair_in[0, h, ru].astype(F32)).astype(BF16)
                    m1[h * U + u].start()

        def add_pair(i, j, hs):
            for h in hs:
                part[j, h] = (part[j, h].astype(F32) + pair_in[i, h].astype(F32)).astype(BF16)

        for j in range(NB):
            wait_w(j)
        with scope("rs_mm1"):
            other(0)
            other(1)
            if early:
                other(2)
            mine(0)
        with scope("rs_wait1"):
            pair[0].wait_recv()
            opposite(0)
        with scope("rs_mm2"):
            if early:
                mine(1)
                opposite(1)
            else:
                other(2)
                opposite(1)
                mine(1)
            mine(2)
        with scope("rs_send2"):
            pair[1].wait_recv()
            add_pair(1, jr, (1,))
            m2[0].start()
            pair[2].wait_recv()
            add_pair(2, jl, (0,))
            m2[1].start()
            add_pair(1, jr, (0,))
            add_pair(2, jl, (1,))
        with scope("rs_mm3"):
            other(3)
            mine(3)
            then()
        with scope("rs_relay"):
            m3 = []
            for u in range(U):
                for h in SIDES:
                    ru = half_rows(u)
                    j = jnp.where(h == 0, jr, jl)
                    remote(relay_in.at[h, ru], relay_in.at[h, ru], rl_s.at[h * U + u], rl_r.at[h * U + u], partner).wait_recv()
                    part[j, h, ru] = (part[j, h, ru].astype(F32) + relay_in[h, ru].astype(F32)).astype(BF16)
                    k = 2 + h * U + u
                    d = remote(part.at[j, h, ru], rs_in.at[2 + h, ru], rs_s.at[k], rs_r.at[k], side_dev(h))
                    d.start()
                    m3.append((h, u, d))
        own = (c * R + x) * 2
        with scope("rs_sum"):
            pair[3].wait_recv()
            for h in range(2):
                sown[h] = part[jx, h].astype(F32) + pair_in[3, h].astype(F32)
            for h in range(2):
                m2[1 - h].wait_recv()
                sown[h] = sown[h] + rs_in[1 - h].astype(F32)
        with scope("rs_fin"):
            first = []
            for h, u, d in m3:
                d.wait_recv()
                ru = half_rows(u)
                hbuf[own + h, ru] = (hbuf[own + h, ru].astype(F32) + (sown[h, ru] + rs_in[2 + h, ru].astype(F32))).astype(BF16)
                ref = hbuf.at[own + h, ru]
                k = h * U + u
                a = remote(ref, ref, ag_s.at[k], ag_r.at[k], side_dev(h))
                a.start()
                first.append((h, u, a))
        done = pair + m1 + m2 + [d for _, _, d in m3]
        return first, done

    def gather(first, done, stats, use):
        own = (c * R + x) * 2
        own2 = hbuf.at[pl.ds(own, 2)]
        p0 = remote(own2, own2, ad_s.at[0], ad_r.at[0], partner)
        p0.start()
        done = done + [p0]
        st = []
        with scope("stats"):
            if stats:
                q = None
                for h in range(2):
                    for a, b in halves(PW):
                        v = hbuf[own + h, :, a:b].astype(F32)
                        q = v * v if q is None else q + v * v
                sq = jnp.broadcast_to(jnp.sum(q.T, axis=0, keepdims=True), (8, n))
                stat[0] = sq
                for k in (4, 3, 5, 2, 6, 1, 7):
                    d = remote(stat.at[0], stat.at[k], st_s.at[k - 1], st_r.at[k - 1], peers[k - 1])
                    d.start()
                    st.append(d)
        with scope("ag_send2"):
            def piece(b, h):
                return hbuf.at[(c * R + b) * 2 + h]
            second = [remote(piece(x, 1), piece(x, 1), ag_s.at[2 * U], ag_r.at[2 * U], right),
                      remote(piece(x, 0), piece(x, 0), ag_s.at[2 * U + 1], ag_r.at[2 * U + 1], left)]
            for d in second:
                d.start()

        fw = []

        def forward(k, ref):
            d = remote(ref, ref, ad_s.at[k], ad_r.at[k], partner)
            d.start()
            fw.append(d)

        relay = []
        with scope("ag_relay"):
            for h, u, a in first:
                a.wait_recv()
                b = jnp.where(h == 0, lb, rb)
                ref = hbuf.at[(c * R + b) * 2 + h, half_rows(u)]
                k = 2 + 2 * U + h * U + u
                d = remote(ref, ref, ag_s.at[k], ag_r.at[k], side_dev(h))
                d.start()
                relay.append((h, u, d))
                forward(3 + h * U + u, ref)
        with scope("ag_stats"):
            if stats:
                for d in st:
                    d.wait_recv()
                t = stat[0]
                for k in range(1, NB):
                    t = t + stat[k]
                put_scale(lax.rsqrt(t[0:1] * (1.0 / D) + EPS))
        with scope("use0"):
            p0.wait_recv()
            use(0)
        with scope("ag_2"):
            second[0].wait_recv()
            forward(1, piece(lb, 1))
            second[1].wait_recv()
            forward(2, piece(rb, 0))
        with scope("use1"):
            use(1)
        with scope("ag_3"):
            for h, u, d in relay:
                d.wait_recv()
                forward(3 + 2 * U + h * U + u, hbuf.at[(c * R + ob) * 2 + h, half_rows(u)])
        with scope("ag_fw1"):
            for d in fw[:2 * U + 2]:
                d.wait_recv()
        with scope("use2"):
            use(2)
        with scope("ag_fw2"):
            for d in fw[2 * U + 2:]:
                d.wait_recv()
        with scope("use3"):
            use(3)
        with scope("ag_drain"):
            for d in done + [d for _, _, d in first + relay] + second + fw + st:
                d.wait_send()

    def qkv_use(l):
        def use(g):
            js = GROUPS[g]
            for j in js:
                normalize(l, ga_ref, j)
            for j in js:
                cp_q(l, j).wait()
            for n0, nw in tiles(NQ):
                accumulate(5 * grp + n0 // LW, group_dot(wq, js, n0, nw), g == 0)
        return use

    quad_row = lax.broadcasted_iota(jnp.int32, (4 * grp, S), 0)
    low = quad_row < 2 * grp
    even = (quad_row // grp) % 2 == 0

    def four(s, t):
        a = kv[s, t:t + 2].reshape(2 * S, hd)
        b = kv[s, t + 2:t + 4].reshape(2 * S, hd)
        return jnp.concatenate([a, b], axis=1)

    scale = hd ** -0.5
    CH = NR // 4

    def attention(l):
        def rope(t):
            return (t * cosb[...] + pltpu.roll(t, hd // 2, 1) * sinb[...]).astype(BF16).astype(F32)

        def head(i):
            return pool[unit(5 * grp + i), :].astype(BF16).astype(F32)

        with scope("rope"):
            kn = rope(head(grp))
            vn = head(grp + 1)
            for g in range(grp):
                qrow[pl.ds(g, n, stride=grp), :] = rope(head(g))
                krow[pl.ds(g, n, stride=grp), :] = kn
                vrow[pl.ds(g, n, stride=grp), :] = vn

        with scope("qk"):
            for s in range(SLOTS):
                if s % SLOTS_PER_STEP == 0:
                    for s2 in range(s, s + SLOTS_PER_STEP):
                        cp_k(l, s2).wait()
                for t in range(0, T, 4):
                    r0 = (s * T + t) * grp
                    q4 = qrow[pl.ds(r0, 4 * grp), :]
                    q4 = jnp.concatenate([jnp.where(low, q4, 0.0), jnp.where(low, 0.0, q4)], axis=1).astype(BF16)
                    o = _dot_nt(q4, four(s, t))
                    arow[pl.ds(r0, 4 * grp), :] = jnp.where(even, o[:, :S], o[:, S:])
                cp_v(l, s).start()

        if l == 0:
            for j in range(NB):
                cp_o(0, j).start()

        with scope("softmax"):
            for ch in range(4):
                rs = slice(ch * CH, (ch + 1) * CH)
                pos = lax.broadcasted_iota(jnp.int32, (CH, S), 1).astype(F32)
                sc = jnp.where(pos < lrow[rs, :], arow[rs, :] * scale, -jnp.inf)
                s_n = jnp.sum(qrow[rs, :] * krow[rs, :], axis=-1, keepdims=True) * scale
                m = jnp.maximum(jnp.max(sc, axis=-1, keepdims=True), s_n)
                p_c = jnp.exp(sc - m)
                p_n = jnp.exp(s_n - m)
                den = jnp.sum(p_c, axis=-1, keepdims=True) + p_n
                prow[rs, :] = p_c
                krow[rs, :] = jnp.broadcast_to(den, (CH, S))
                vrow[rs, :] = vrow[rs, :] * p_n

        with scope("pv"):
            for s in range(SLOTS):
                if s % SLOTS_PER_STEP == 0:
                    for s2 in range(s, s + SLOTS_PER_STEP):
                        cp_v(l, s2).wait()
                for t in range(0, T, 4):
                    r0 = (s * T + t) * grp
                    p4 = prow[pl.ds(r0, 4 * grp), :]
                    p4 = jnp.concatenate([jnp.where(even, p4, 0.0), jnp.where(even, 0.0, p4)], axis=1).astype(BF16)
                    o = _dot(p4, four(s, t))
                    arow[pl.ds(r0, 4 * grp), :] = jnp.where(low, o[:, :hd], o[:, hd:])

        with scope("att_out"):
            for ch in range(4):
                rs = slice(ch * CH, (ch + 1) * CH)
                arow[rs, :] = (arow[rs, :] + vrow[rs, :]) / krow[rs, :]
            for g in range(grp):
                att[:, g * hd:(g + 1) * hd] = arow[pl.ds(g, n, stride=grp), :].astype(BF16)

    def mlp_use(l):
        FU = F // LW

        def use(g):
            js = GROUPS[g]
            for j in js:
                normalize(l, gm_ref, j)
            for j in js:
                cp_g(l, j).wait()
                cp_u(l, j).wait()
            for n0, nw in tiles(F):
                if g < NG - 1:
                    for k, w in enumerate((wg, wu)):
                        accumulate((k * F + n0) // LW, group_dot(w, js, n0, nw), g == 0)
                else:
                    dg, du = group_dot(wg, js, n0, nw), group_dot(wu, js, n0, nw)
                    for k, (a, b) in enumerate(halves(nw)):
                        u = n0 // LW + k
                        gate = pool[unit(u), :] + dg[:, a:b]
                        up = pool[unit(FU + u), :] + du[:, a:b]
                        act[:, n0 + a:n0 + b] = (jax.nn.silu(gate) * up).astype(BF16)
        return use

    with scope("x_wait"):
        for p in range(2 * NB):
            cp_x(p).wait()
    with scope("scale0"):
        for j in blocks[2:]:
            cp_q(0, j).start()
        local_scale()
        for d in small:
            d.wait()

    outs = []

    def out_use(g):
        for j in GROUPS[g]:
            for h in range(2):
                p = j * 2 + h
                d = pltpu.make_async_copy(hbuf.at[p], y_hbm.at[:, cols(p * PW, PW)], s_y.at[g * 4 + len(outs) % 4])
                d.start()
                outs.append(d)

    pending = None
    for l in range(L):
        if pending is None:
            for g in range(NG):
                with scope("qkv"):
                    qkv_use(l)(g)
                if g == 0:
                    with scope("tables"):
                        tables()
                if g == 1:
                    for s in range(SLOTS // 2):
                        cp_k(0, s).start()
                if g == 2:
                    for s in range(SLOTS // 2, SLOTS):
                        cp_k(0, s).start()
        else:
            gather(*pending, True, qkv_use(l))
        attention(l)
        if l == 0:
            pl.semaphore_wait(barrier, NB - 1)

        def mlp_weights(l=l):
            if l == 0:
                for j in blocks:
                    cp_g(0, j).start()
                    cp_u(0, j).start()
                for j in range(NB):
                    cp_d(0, j).start()

        pending = reduce_scatter(lambda j: _dot(att[...], wo[:, cols(j * BW, BW)]), lambda j: cp_o(l, j).wait(), True, mlp_weights)
        if l + 1 < L:
            for j in range(NB):
                cp_o(l + 1, j).start()
        gather(*pending, True, mlp_use(l))
        if l + 1 < L:
            for j in blocks:
                cp_q(l + 1, j).start()
            for s in range(SLOTS):
                cp_k(l + 1, s).start()
            for j in blocks:
                cp_g(l + 1, j).start()
                cp_u(l + 1, j).start()
        pending = reduce_scatter(lambda j: _dot(act[...], wd[:, cols(j * BW, BW)]), lambda j: cp_d(l, j).wait(), False, lambda: None)
        if l + 1 < L:
            for j in range(NB):
                cp_d(l + 1, j).start()
    gather(*pending, False, out_use)
    with scope("y_out"):
        for d in outs:
            d.wait()


def solution(mesh):
    tp = mesh.shape["tp"]

    def body(x, g_attn, w_qkv, w_o, g_mlp, w_gate, w_up, w_down, k_cache, v_cache, lengths):
        n, D = x.shape
        L, _, NQ = w_qkv.shape
        KO, F = w_o.shape[1], w_gate.shape[2]
        S, hd = k_cache.shape[2], k_cache.shape[4]
        R = tp // 2
        NB, PW, BW = tp, D // tp // 2, D // tp
        grp = KO // hd
        kc = k_cache.reshape(L, n, S, hd)
        vc = v_cache.reshape(L, n, S, hd)
        half = hd // 2
        inv = np.float32(ROPE_THETA) ** (-np.arange(half, dtype=np.float32) * np.float32(2.0) / np.float32(hd))
        inv = jnp.asarray(np.concatenate([inv, inv])[None, :].astype(np.float32))
        dims = (L, n, D, NQ, KO, F, S, hd, R)
        anyspec = pl.BlockSpec(memory_space=pl.ANY)
        V = pltpu.VMEM
        DMA = pltpu.SemaphoreType.DMA
        rows = n * grp
        scratch = [
            V((D, NQ), BF16), V((KO, D), BF16), V((D, F), BF16), V((D, F), BF16), V((F, D), BF16),
            V((SLOTS, n // SLOTS, S, hd), BF16),
            V((2 * NB, n, PW), BF16), V((2 * NB, n, PW), BF16),
            V((NB, 2, n, PW), BF16), V((R, 2, n, PW), BF16), V((2, n, PW), BF16), V((4, n, PW), BF16), V((2, n, PW), F32),
            V((max(2 * F // 128, 5 * grp + NQ // 128) * n, 128), F32), V((n, F), BF16),
            V((rows, hd), F32), V((n, hd), F32), V((n, hd), F32), V((n, KO), BF16), V((n, 128), F32), V((NB, 8, n), F32),
            V((L, D), BF16), V((L, D), BF16), V((1, n), jnp.int32), V((1, hd), F32), DMA((4,)),
            DMA((2 * NB,)), DMA((NB,)), DMA((NB,)), DMA((NB,)), DMA((NB,)), DMA((NB,)), DMA((SLOTS,)), DMA((2 * NB,)),
            DMA((4,)), DMA((4,)), DMA((2 * U,)), DMA((2 * U,)), DMA((2 + 2 * U,)), DMA((2 + 2 * U,)),
            DMA((2 + 4 * U,)), DMA((2 + 4 * U,)), DMA((3 + 4 * U,)), DMA((3 + 4 * U,)),
            DMA((NB - 1,)), DMA((NB - 1,)),
        ]
        y = pl.pallas_call(
            functools.partial(_kernel, dims),
            out_shape=jax.ShapeDtypeStruct((n, D), BF16),
            in_specs=[anyspec] * 12,
            out_specs=anyspec,
            scratch_shapes=scratch,
            compiler_params=pltpu.CompilerParams(collective_id=0, has_side_effects=True, vmem_limit_bytes=67043328),
        )(x, g_attn, w_qkv, w_o, g_mlp, w_gate, w_up, w_down, kc, vc, lengths.reshape(1, n), inv)
        return y

    col = P(None, None, 'tp')
    row = P(None, 'tp', None)
    cache = P(None, 'dp', None, 'tp', None)
    return jax.shard_map(body, mesh=mesh,
                         in_specs=(P('dp', None), P(), col, row, P(), col, col, row, cache, cache, P('dp')),
                         out_specs=P('dp', None), check_vma=False)
```

```python
import functools

import jax
import jax.numpy as jnp
import numpy as np
from jax import lax
from jax.experimental import pallas as pl
from jax.experimental.pallas import tpu as pltpu
from jax.sharding import PartitionSpec as P

EPS = 1e-5
ROPE_THETA = 500000.0
F32 = jnp.float32
BF16 = jnp.bfloat16
SLOTS = 8
SLOTS_PER_STEP = 4
U = 4
RS_ORDER = (2, 1, 3, 0)


def _dot(a, b):
    return jnp.dot(a, b, preferred_element_type=F32)


def _dot_nt(a, b):
    return lax.dot_general(a, b, (((1,), (1,)), ((), ())), preferred_element_type=F32)


def _kernel(dims, x_hbm, ga_hbm, wqkv_hbm, wo_hbm, gm_hbm, wg_hbm, wu_hbm, wd_hbm, kc_hbm, vc_hbm, len_hbm, inv_hbm,
            y_hbm,
            wq, wo, wg, wu, wd, kv, hbuf, abuf, part, pair_in, relay_in, rs_in, sown, pool, act, lrow, cosb, sinb, att, rbuf, stat, ga_ref, gm_ref, len_ref, inv_ref, s_c,
            s_x, s_q, s_o, s_g, s_u, s_d, s_kv, s_y,
            pr_s, pr_r, rl_s, rl_r, rs_s, rs_r, ag_s, ag_r, ad_s, ad_r, ax_s, ax_r, st_s, st_r):
    L, n, D, NQ, KO, F, S, hd, R = dims
    NB = 2 * R
    BW = D // NB
    PW = BW // 2
    grp = KO // hd
    T = n // SLOTS
    LW = 128
    NR = n * grp
    qrow, krow, vrow, arow, prow = (pool.at[pl.ds(i * NR, NR)] for i in range(5))
    tp = lax.axis_index("tp")
    x = tp // 2
    c = tp % 2
    right = {"tp": ((x + 1) % R) * 2 + c}
    left = {"tp": ((x + R - 1) % R) * 2 + c}
    partner = {"tp": x * 2 + (1 - c)}
    MESH = pl.DeviceIdType.MESH

    def chip(off):
        return (x + off) % R

    def cols(start, size):
        return pl.ds(pl.multiple_of(start, 128), size)

    def rows(start, size):
        return pl.ds(pl.multiple_of(start, 128), size)

    def cp_x(p):
        return pltpu.make_async_copy(x_hbm.at[:, cols(p * PW, PW)], hbuf.at[p], s_x.at[p])

    def cp_q(l, j):
        return pltpu.make_async_copy(wqkv_hbm.at[l, rows(j * BW, BW), :], wq.at[rows(j * BW, BW), :], s_q.at[j])

    def cp_o(l, j):
        return pltpu.make_async_copy(wo_hbm.at[l, :, cols(j * BW, BW)], wo.at[:, cols(j * BW, BW)], s_o.at[j])

    def cp_g(l, j):
        return pltpu.make_async_copy(wg_hbm.at[l, rows(j * BW, BW), :], wg.at[rows(j * BW, BW), :], s_g.at[j])

    def cp_u(l, j):
        return pltpu.make_async_copy(wu_hbm.at[l, rows(j * BW, BW), :], wu.at[rows(j * BW, BW), :], s_u.at[j])

    def cp_d(l, j):
        return pltpu.make_async_copy(wd_hbm.at[l, :, cols(j * BW, BW)], wd.at[:, cols(j * BW, BW)], s_d.at[j])

    def cp_k(l, s):
        return pltpu.make_async_copy(kc_hbm.at[l, pl.ds(s * T, T)], kv.at[s], s_kv.at[s])

    def cp_v(l, s):
        return pltpu.make_async_copy(vc_hbm.at[l, pl.ds(s * T, T)], kv.at[s], s_kv.at[s])

    scope = jax.named_scope
    barrier = pltpu.get_barrier_semaphore()
    peers = [{"tp": (tp + k) % NB} for k in range(1, NB)]

    lb, rb, ob = chip(3), chip(1), chip(2)
    GROUPS = ((c * R + x, (1 - c) * R + x), (c * R + lb, c * R + rb), ((1 - c) * R + lb, (1 - c) * R + rb),
              (c * R + ob, (1 - c) * R + ob))
    NG = len(GROUPS)
    blocks = [j for g in GROUPS for j in g]

    for p in range(2 * NB):
        cp_x(p).start()
    small = [pltpu.make_async_copy(a, b, s_c.at[i])
             for i, (a, b) in enumerate(((len_hbm, len_ref), (inv_hbm, inv_ref), (ga_hbm, ga_ref), (gm_hbm, gm_ref)))]
    for d in small:
        d.start()
    for j in blocks[:2]:
        cp_q(0, j).start()
    for d in peers:
        pl.semaphore_signal(barrier, inc=1, device_id=d, device_id_type=MESH)

    def tables():
        lcol = jnp.broadcast_to(len_ref[...].astype(F32), (hd, n)).T
        ang = lcol * inv_ref[...]
        lane = lax.broadcasted_iota(jnp.int32, (n, hd), 1)
        cosb[...] = jnp.cos(ang)
        sn = jnp.sin(ang)
        sinb[...] = jnp.where(lane < hd // 2, -sn, sn)
        for g in range(grp):
            lrow[pl.ds(g, n, stride=grp), :] = lcol

    def remote(src, dst, ss, rs, dev):
        return pltpu.make_async_remote_copy(src_ref=src, dst_ref=dst, send_sem=ss, recv_sem=rs, device_id=dev,
                                            device_id_type=MESH)

    def halves(width):
        return [(k, k + LW) for k in range(0, width, LW)]

    def put_scale(row):
        rbuf[...] = jnp.broadcast_to(row, (LW, n)).T

    def local_scale():
        def sq(p, s):
            v = hbuf[p].astype(F32)
            return s + v * v
        s = lax.fori_loop(0, 2 * NB, sq, jnp.zeros((n, PW), F32))
        r = lax.rsqrt(jnp.sum(s, axis=-1, keepdims=True) * (1.0 / D) + EPS)
        rbuf[...] = jnp.broadcast_to(r, (n, LW))

    def normalize(l, ref, j):
        for h in range(2):
            p = j * 2 + h
            for a, b in halves(PW):
                g = ref[l:l + 1, cols(p * PW + a, LW)].astype(F32)
                abuf[p, :, a:b] = (hbuf[p, :, a:b].astype(F32) * rbuf[...] * g).astype(BF16)

    def group_dot(w, js, n0, nw):
        s = None
        for j in js:
            for h in range(2):
                d = _dot(abuf[j * 2 + h], w[rows(j * BW + h * PW, PW), n0:n0 + nw])
                s = d if s is None else s + d
        return s

    def unit(i):
        return pl.ds(i * n, n)

    def tiles(width):
        return [(n0, min(256, width - n0)) for n0 in range(0, width, 256)]

    def accumulate(u, d, first):
        for k, (a, b) in enumerate(halves(d.shape[1])):
            if first:
                pool[unit(u + k), :] = d[:, a:b]
            else:
                pool[unit(u + k), :] += d[:, a:b]

    UH = n // U
    slow = jnp.where(x == 0, 1, 0)
    SIDES = (slow, 1 - slow)
    right_i, left_i = right["tp"], left["tp"]

    def side_dev(h):
        return {"tp": jnp.where(h == 0, right_i, left_i)}

    def half_rows(u):
        return pl.ds(u * UH, UH)

    def reduce_scatter(block, wait_w, early, then):
        pair = []

        def other(i):
            j = (1 - c) * R + chip(RS_ORDER[i])
            o = block(j).astype(BF16)
            part[j, 0] = o[:, :PW]
            part[j, 1] = o[:, PW:]
            d = remote(part.at[j], pair_in.at[i], pr_s.at[i], pr_r.at[i], partner)
            d.start()
            pair.append(d)

        def mine(i):
            j = c * R + chip(RS_ORDER[i])
            o = block(j).astype(BF16)
            part[j, 0] = o[:, :PW]
            part[j, 1] = o[:, PW:]

        jo, jr, jl, jx = (c * R + chip(o) for o in RS_ORDER)
        m1 = [remote(part.at[jo, h, half_rows(u)], relay_in.at[h, half_rows(u)], rl_s.at[h * U + u],
                     rl_r.at[h * U + u], (right, left)[h]) for h in range(2) for u in range(U)]
        m2 = [remote(part.at[jr, 1], rs_in.at[0], rs_s.at[0], rs_r.at[0], right),
              remote(part.at[jl, 0], rs_in.at[1], rs_s.at[1], rs_r.at[1], left)]

        def opposite(k):
            for u in range(k * U // 2, (k + 1) * U // 2):
                for h in range(2):
                    ru = half_rows(u)
                    part[jo, h, ru] = (part[jo, h, ru].astype(F32) + pair_in[0, h, ru].astype(F32)).astype(BF16)
                    m1[h * U + u].start()

        def add_pair(i, j, hs):
            for h in hs:
                part[j, h] = (part[j, h].astype(F32) + pair_in[i, h].astype(F32)).astype(BF16)

        for j in range(NB):
            wait_w(j)
        with scope("rs_mm1"):
            other(0)
            other(1)
            if early:
                other(2)
            mine(0)
        with scope("rs_wait1"):
            pair[0].wait_recv()
            opposite(0)
        with scope("rs_mm2"):
            if early:
                mine(1)
                opposite(1)
            else:
                other(2)
                opposite(1)
                mine(1)
            mine(2)
        with scope("rs_send2"):
            pair[1].wait_recv()
            add_pair(1, jr, (1,))
            m2[0].start()
            pair[2].wait_recv()
            add_pair(2, jl, (0,))
            m2[1].start()
            add_pair(1, jr, (0,))
            add_pair(2, jl, (1,))
        with scope("rs_mm3"):
            other(3)
            mine(3)
            then()
        with scope("rs_relay"):
            m3 = []
            for u in range(U):
                for h in SIDES:
                    ru = half_rows(u)
                    j = jnp.where(h == 0, jr, jl)
                    remote(relay_in.at[h, ru], relay_in.at[h, ru], rl_s.at[h * U + u], rl_r.at[h * U + u], partner).wait_recv()
                    part[j, h, ru] = (part[j, h, ru].astype(F32) + relay_in[h, ru].astype(F32)).astype(BF16)
                    k = 2 + h * U + u
                    d = remote(part.at[j, h, ru], rs_in.at[2 + h, ru], rs_s.at[k], rs_r.at[k], side_dev(h))
                    d.start()
                    m3.append((h, u, d))
        own = (c * R + x) * 2
        with scope("rs_sum"):
            pair[3].wait_recv()
            for h in range(2):
                sown[h] = part[jx, h].astype(F32) + pair_in[3, h].astype(F32)
            for h in range(2):
                m2[1 - h].wait_recv()
                sown[h] = sown[h] + rs_in[1 - h].astype(F32)
        with scope("rs_fin"):
            first = []
            for h, u, d in m3:
                d.wait_recv()
                ru = half_rows(u)
                hbuf[own + h, ru] = (hbuf[own + h, ru].astype(F32) + (sown[h, ru] + rs_in[2 + h, ru].astype(F32))).astype(BF16)
                ref = hbuf.at[own + h, ru]
                k = h * U + u
                a = remote(ref, ref, ag_s.at[k], ag_r.at[k], side_dev(h))
                a.start()
                first.append((h, u, a))
        done = pair + m1 + m2 + [d for _, _, d in m3]
        return first, done

    def gather(first, done, stats, use):
        own = (c * R + x) * 2
        own2 = hbuf.at[pl.ds(own, 2)]
        p0 = remote(own2, own2, ad_s.at[0], ad_r.at[0], partner)
        p0.start()
        done = done + [p0]
        st = []
        with scope("stats"):
            if stats:
                q = None
                for h in range(2):
                    for a, b in halves(PW):
                        v = hbuf[own + h, :, a:b].astype(F32)
                        q = v * v if q is None else q + v * v
                sq = jnp.broadcast_to(jnp.sum(q.T, axis=0, keepdims=True), (8, n))
                stat[0] = sq
                for k in (4, 3, 5, 2, 6, 1, 7):
                    d = remote(stat.at[0], stat.at[k], st_s.at[k - 1], st_r.at[k - 1], peers[k - 1])
                    d.start()
                    st.append(d)
        with scope("ag_send2"):
            def piece(b, h):
                return hbuf.at[(c * R + b) * 2 + h]
            second = [remote(piece(x, 1), piece(x, 1), ag_s.at[2 * U], ag_r.at[2 * U], right),
                      remote(piece(x, 0), piece(x, 0), ag_s.at[2 * U + 1], ag_r.at[2 * U + 1], left)]
            for d in second:
                d.start()

        fw = []

        def forward(k, ref):
            d = remote(ref, ref, ad_s.at[k], ad_r.at[k], partner)
            d.start()
            fw.append(d)

        relay = []

        def both_cores(h, u, ref):
            k = h * U + u
            return remote(ref, ref, ax_s.at[k], ax_r.at[k], {"tp": side_dev(h)["tp"] + 1 - 2 * c})

        def last(h, u):
            return hbuf.at[(c * R + ob) * 2 + h, half_rows(u)]

        def last_forward(h, u):
            k = 3 + 2 * U + h * U + u
            return remote(last(h, u), last(h, u), ad_s.at[k], ad_r.at[k], partner)

        with scope("ag_relay"):
            for h, u, a in first:
                a.wait_recv()
                b = jnp.where(h == 0, lb, rb)
                ref = hbuf.at[(c * R + b) * 2 + h, half_rows(u)]
                k = 2 + 2 * U + h * U + u
                d = remote(ref, ref, ag_s.at[k], ag_r.at[k], side_dev(h))
                d.start()
                relay.append((h, u, d))
                forward(3 + h * U + u, ref)
                extra = both_cores(h, u, ref)

                @pl.when(c == 0)
                def _():
                    extra.start()
        with scope("ag_stats"):
            if stats:
                for d in st:
                    d.wait_recv()
                t = stat[0]
                for k in range(1, NB):
                    t = t + stat[k]
                put_scale(lax.rsqrt(t[0:1] * (1.0 / D) + EPS))
        with scope("use0"):
            p0.wait_recv()
            use(0)
        with scope("ag_2"):
            second[0].wait_recv()
            forward(1, piece(lb, 1))
            second[1].wait_recv()
            forward(2, piece(rb, 0))
        with scope("use1"):
            use(1)
        with scope("ag_3"):
            for h, u, d in relay:
                d.wait_recv()
                down = last_forward(h, u)

                @pl.when(c == 1)
                def _():
                    down.start()
        with scope("ag_fw1"):
            for d in fw:
                d.wait_recv()
        with scope("use2"):
            use(2)
        with scope("ag_fw2"):
            @pl.when(c == 0)
            def _():
                for h, u, _ in relay:
                    last_forward(h, u).wait_recv()

            @pl.when(c == 1)
            def _():
                for h, u, _ in relay:
                    both_cores(h, u, last(h, u)).wait_recv()
        with scope("use3"):
            use(3)
        with scope("ag_drain"):
            for d in done + [d for _, _, d in first + relay] + second + fw + st:
                d.wait_send()

            @pl.when(c == 1)
            def _():
                for h, u, _ in relay:
                    last_forward(h, u).wait_send()

            @pl.when(c == 0)
            def _():
                for h, u, _ in relay:
                    both_cores(h, u, last(h, u)).wait_send()

    def qkv_use(l):
        def use(g):
            js = GROUPS[g]
            for j in js:
                normalize(l, ga_ref, j)
            for j in js:
                cp_q(l, j).wait()
            for n0, nw in tiles(NQ):
                accumulate(5 * grp + n0 // LW, group_dot(wq, js, n0, nw), g == 0)
        return use

    quad_row = lax.broadcasted_iota(jnp.int32, (4 * grp, S), 0)
    low = quad_row < 2 * grp
    even = (quad_row // grp) % 2 == 0

    def four(s, t):
        a = kv[s, t:t + 2].reshape(2 * S, hd)
        b = kv[s, t + 2:t + 4].reshape(2 * S, hd)
        return jnp.concatenate([a, b], axis=1)

    scale = hd ** -0.5
    CH = NR // 4

    def attention(l):
        def rope(t):
            return (t * cosb[...] + pltpu.roll(t, hd // 2, 1) * sinb[...]).astype(BF16).astype(F32)

        def head(i):
            return pool[unit(5 * grp + i), :].astype(BF16).astype(F32)

        with scope("rope"):
            kn = rope(head(grp))
            vn = head(grp + 1)
            for g in range(grp):
                qrow[pl.ds(g, n, stride=grp), :] = rope(head(g))
                krow[pl.ds(g, n, stride=grp), :] = kn
                vrow[pl.ds(g, n, stride=grp), :] = vn

        with scope("qk"):
            for s in range(SLOTS):
                if s % SLOTS_PER_STEP == 0:
                    for s2 in range(s, s + SLOTS_PER_STEP):
                        cp_k(l, s2).wait()
                for t in range(0, T, 4):
                    r0 = (s * T + t) * grp
                    q4 = qrow[pl.ds(r0, 4 * grp), :]
                    q4 = jnp.concatenate([jnp.where(low, q4, 0.0), jnp.where(low, 0.0, q4)], axis=1).astype(BF16)
                    o = _dot_nt(q4, four(s, t))
                    arow[pl.ds(r0, 4 * grp), :] = jnp.where(even, o[:, :S], o[:, S:])
                cp_v(l, s).start()

        with scope("softmax"):
            for ch in range(4):
                rs = slice(ch * CH, (ch + 1) * CH)
                pos = lax.broadcasted_iota(jnp.int32, (CH, S), 1).astype(F32)
                sc = jnp.where(pos < lrow[rs, :], arow[rs, :] * scale, -jnp.inf)
                s_n = jnp.sum(qrow[rs, :] * krow[rs, :], axis=-1, keepdims=True) * scale
                m = jnp.maximum(jnp.max(sc, axis=-1, keepdims=True), s_n)
                p_c = jnp.exp(sc - m)
                p_n = jnp.exp(s_n - m)
                den = jnp.sum(p_c, axis=-1, keepdims=True) + p_n
                prow[rs, :] = p_c
                krow[rs, :] = jnp.broadcast_to(den, (CH, S))
                vrow[rs, :] = vrow[rs, :] * p_n

        with scope("pv"):
            for s in range(SLOTS):
                if s % SLOTS_PER_STEP == 0:
                    for s2 in range(s, s + SLOTS_PER_STEP):
                        cp_v(l, s2).wait()
                for t in range(0, T, 4):
                    r0 = (s * T + t) * grp
                    p4 = prow[pl.ds(r0, 4 * grp), :]
                    p4 = jnp.concatenate([jnp.where(even, p4, 0.0), jnp.where(even, 0.0, p4)], axis=1).astype(BF16)
                    o = _dot(p4, four(s, t))
                    arow[pl.ds(r0, 4 * grp), :] = jnp.where(low, o[:, :hd], o[:, hd:])

        with scope("att_out"):
            for ch in range(4):
                rs = slice(ch * CH, (ch + 1) * CH)
                arow[rs, :] = (arow[rs, :] + vrow[rs, :]) / krow[rs, :]
            for g in range(grp):
                att[:, g * hd:(g + 1) * hd] = arow[pl.ds(g, n, stride=grp), :].astype(BF16)

    def mlp_use(l):
        FU = F // LW

        def use(g):
            js = GROUPS[g]
            for j in js:
                normalize(l, gm_ref, j)
            for j in js:
                cp_g(l, j).wait()
                cp_u(l, j).wait()
            for n0, nw in tiles(F):
                if g < NG - 1:
                    for k, w in enumerate((wg, wu)):
                        accumulate((k * F + n0) // LW, group_dot(w, js, n0, nw), g == 0)
                else:
                    dg, du = group_dot(wg, js, n0, nw), group_dot(wu, js, n0, nw)
                    for k, (a, b) in enumerate(halves(nw)):
                        u = n0 // LW + k
                        gate = pool[unit(u), :] + dg[:, a:b]
                        up = pool[unit(FU + u), :] + du[:, a:b]
                        act[:, n0 + a:n0 + b] = (jax.nn.silu(gate) * up).astype(BF16)
        return use

    with scope("x_wait"):
        for p in range(2 * NB):
            cp_x(p).wait()
    with scope("scale0"):
        for j in blocks[2:]:
            cp_q(0, j).start()
        for s in range(SLOTS // 2):
            cp_k(0, s).start()
        local_scale()
        for d in small:
            d.wait()

    outs = []

    def out_use(g):
        for j in GROUPS[g]:
            for h in range(2):
                p = j * 2 + h
                d = pltpu.make_async_copy(hbuf.at[p], y_hbm.at[:, cols(p * PW, PW)], s_y.at[g * 4 + len(outs) % 4])
                d.start()
                outs.append(d)

    pending = None
    for l in range(L):
        if pending is None:
            for g in range(NG):
                with scope("qkv"):
                    qkv_use(l)(g)
                if g == 0:
                    with scope("tables"):
                        tables()
                if g == 0:
                    for s in range(SLOTS // 2, SLOTS):
                        cp_k(0, s).start()
                if g == 2:
                    for j in range(NB):
                        cp_o(0, j).start()
        else:
            gather(*pending, True, qkv_use(l))
        attention(l)
        if l == 0:
            pl.semaphore_wait(barrier, NB - 1)

        def mlp_weights(l=l):
            if l == 0:
                for j in blocks:
                    cp_g(0, j).start()
                    cp_u(0, j).start()
                for j in range(NB):
                    cp_d(0, j).start()

        pending = reduce_scatter(lambda j: _dot(att[...], wo[:, cols(j * BW, BW)]), lambda j: cp_o(l, j).wait(), True, mlp_weights)
        if l + 1 < L:
            for j in range(NB):
                cp_o(l + 1, j).start()
        gather(*pending, True, mlp_use(l))
        if l + 1 < L:
            for j in blocks:
                cp_q(l + 1, j).start()
            for s in range(SLOTS):
                cp_k(l + 1, s).start()
            for j in blocks:
                cp_g(l + 1, j).start()
                cp_u(l + 1, j).start()
        pending = reduce_scatter(lambda j: _dot(act[...], wd[:, cols(j * BW, BW)]), lambda j: cp_d(l, j).wait(), False, lambda: None)
        if l + 1 < L:
            for j in range(NB):
                cp_d(l + 1, j).start()
    gather(*pending, False, out_use)
    with scope("y_out"):
        for d in outs:
            d.wait()


def solution(mesh):
    tp = mesh.shape["tp"]

    def body(x, g_attn, w_qkv, w_o, g_mlp, w_gate, w_up, w_down, k_cache, v_cache, lengths):
        n, D = x.shape
        L, _, NQ = w_qkv.shape
        KO, F = w_o.shape[1], w_gate.shape[2]
        S, hd = k_cache.shape[2], k_cache.shape[4]
        R = tp // 2
        NB, PW, BW = tp, D // tp // 2, D // tp
        grp = KO // hd
        kc = k_cache.reshape(L, n, S, hd)
        vc = v_cache.reshape(L, n, S, hd)
        half = hd // 2
        inv = np.float32(ROPE_THETA) ** (-np.arange(half, dtype=np.float32) * np.float32(2.0) / np.float32(hd))
        inv = jnp.asarray(np.concatenate([inv, inv])[None, :].astype(np.float32))
        dims = (L, n, D, NQ, KO, F, S, hd, R)
        anyspec = pl.BlockSpec(memory_space=pl.ANY)
        V = pltpu.VMEM
        DMA = pltpu.SemaphoreType.DMA
        rows = n * grp
        scratch = [
            V((D, NQ), BF16), V((KO, D), BF16), V((D, F), BF16), V((D, F), BF16), V((F, D), BF16),
            V((SLOTS, n // SLOTS, S, hd), BF16),
            V((2 * NB, n, PW), BF16), V((2 * NB, n, PW), BF16),
            V((NB, 2, n, PW), BF16), V((R, 2, n, PW), BF16), V((2, n, PW), BF16), V((4, n, PW), BF16), V((2, n, PW), F32),
            V((max(2 * F // 128, 5 * grp + NQ // 128) * n, 128), F32), V((n, F), BF16),
            V((rows, hd), F32), V((n, hd), F32), V((n, hd), F32), V((n, KO), BF16), V((n, 128), F32), V((NB, 8, n), F32),
            V((L, D), BF16), V((L, D), BF16), V((1, n), jnp.int32), V((1, hd), F32), DMA((4,)),
            DMA((2 * NB,)), DMA((NB,)), DMA((NB,)), DMA((NB,)), DMA((NB,)), DMA((NB,)), DMA((SLOTS,)), DMA((2 * NB,)),
            DMA((4,)), DMA((4,)), DMA((2 * U,)), DMA((2 * U,)), DMA((2 + 2 * U,)), DMA((2 + 2 * U,)),
            DMA((2 + 4 * U,)), DMA((2 + 4 * U,)), DMA((3 + 4 * U,)), DMA((3 + 4 * U,)), DMA((2 * U,)), DMA((2 * U,)),
            DMA((NB - 1,)), DMA((NB - 1,)),
        ]
        y = pl.pallas_call(
            functools.partial(_kernel, dims),
            out_shape=jax.ShapeDtypeStruct((n, D), BF16),
            in_specs=[anyspec] * 12,
            out_specs=anyspec,
            scratch_shapes=scratch,
            compiler_params=pltpu.CompilerParams(collective_id=0, has_side_effects=True, vmem_limit_bytes=67043328),
        )(x, g_attn, w_qkv, w_o, g_mlp, w_gate, w_up, w_down, kc, vc, lengths.reshape(1, n), inv)
        return y

    col = P(None, None, 'tp')
    row = P(None, 'tp', None)
    cache = P(None, 'dp', None, 'tp', None)
    return jax.shard_map(body, mesh=mesh,
                         in_specs=(P('dp', None), P(), col, row, P(), col, col, row, cache, cache, P('dp')),
                         out_specs=P('dp', None), check_vma=False)
```

```python
import functools

import jax
import jax.numpy as jnp
import numpy as np
from jax import lax
from jax.experimental import pallas as pl
from jax.experimental.pallas import tpu as pltpu
from jax.sharding import PartitionSpec as P

EPS = 1e-5
ROPE_THETA = 500000.0
F32 = jnp.float32
BF16 = jnp.bfloat16
SLOTS = 8
SLOTS_PER_STEP = 4
U = 4
RS_ORDER = (2, 1, 3, 0)


def _dot(a, b):
    return jnp.dot(a, b, preferred_element_type=F32)


def _dot_nt(a, b):
    return lax.dot_general(a, b, (((1,), (1,)), ((), ())), preferred_element_type=F32)


def _kernel(dims, x_hbm, ga_hbm, wqkv_hbm, wo_hbm, gm_hbm, wg_hbm, wu_hbm, wd_hbm, kc_hbm, vc_hbm, len_hbm, inv_hbm,
            y_hbm,
            wq, wo, wg, wu, wd, kv, hbuf, abuf, part, pair_in, relay_in, rs_in, sown, pool, act, lrow, cosb, sinb, att, rbuf, stat, ga_ref, gm_ref, len_ref, inv_ref, s_c,
            s_x, s_q, s_o, s_g, s_u, s_d, s_kv, s_y,
            pr_s, pr_r, rl_s, rl_r, rs_s, rs_r, ag_s, ag_r, ad_s, ad_r, ax_s, ax_r, st_s, st_r):
    L, n, D, NQ, KO, F, S, hd, R = dims
    NB = 2 * R
    BW = D // NB
    PW = BW // 2
    grp = KO // hd
    T = n // SLOTS
    LW = 128
    NR = n * grp
    qrow, krow, vrow, arow, prow = (pool.at[pl.ds(i * NR, NR)] for i in range(5))
    tp = lax.axis_index("tp")
    x = tp // 2
    c = tp % 2
    right = {"tp": ((x + 1) % R) * 2 + c}
    left = {"tp": ((x + R - 1) % R) * 2 + c}
    partner = {"tp": x * 2 + (1 - c)}
    MESH = pl.DeviceIdType.MESH

    def chip(off):
        return (x + off) % R

    def cols(start, size):
        return pl.ds(pl.multiple_of(start, 128), size)

    def rows(start, size):
        return pl.ds(pl.multiple_of(start, 128), size)

    def cp_x(p):
        return pltpu.make_async_copy(x_hbm.at[:, cols(p * PW, PW)], hbuf.at[p], s_x.at[p])

    def cp_q(l, j):
        return pltpu.make_async_copy(wqkv_hbm.at[l, rows(j * BW, BW), :], wq.at[rows(j * BW, BW), :], s_q.at[j])

    def cp_o(l, j):
        return pltpu.make_async_copy(wo_hbm.at[l, :, cols(j * BW, BW)], wo.at[:, cols(j * BW, BW)], s_o.at[j])

    def cp_g(l, j):
        return pltpu.make_async_copy(wg_hbm.at[l, rows(j * BW, BW), :], wg.at[rows(j * BW, BW), :], s_g.at[j])

    def cp_u(l, j):
        return pltpu.make_async_copy(wu_hbm.at[l, rows(j * BW, BW), :], wu.at[rows(j * BW, BW), :], s_u.at[j])

    def cp_d(l, j):
        return pltpu.make_async_copy(wd_hbm.at[l, :, cols(j * BW, BW)], wd.at[:, cols(j * BW, BW)], s_d.at[j])

    def cp_k(l, s):
        return pltpu.make_async_copy(kc_hbm.at[l, pl.ds(s * T, T)], kv.at[s], s_kv.at[s])

    def cp_v(l, s):
        return pltpu.make_async_copy(vc_hbm.at[l, pl.ds(s * T, T)], kv.at[s], s_kv.at[s])

    scope = jax.named_scope
    barrier = pltpu.get_barrier_semaphore()
    peers = [{"tp": (tp + k) % NB} for k in range(1, NB)]

    lb, rb, ob = chip(3), chip(1), chip(2)
    GROUPS = ((c * R + x, (1 - c) * R + x), (c * R + lb, c * R + rb), ((1 - c) * R + lb, (1 - c) * R + rb),
              (c * R + ob, (1 - c) * R + ob))
    NG = len(GROUPS)
    blocks = [j for g in GROUPS for j in g]

    for p in range(2 * NB):
        cp_x(p).start()
    small = [pltpu.make_async_copy(a, b, s_c.at[i])
             for i, (a, b) in enumerate(((len_hbm, len_ref), (inv_hbm, inv_ref), (ga_hbm, ga_ref), (gm_hbm, gm_ref)))]
    for d in small:
        d.start()
    for j in blocks[:4]:
        cp_q(0, j).start()
    for d in peers:
        pl.semaphore_signal(barrier, inc=1, device_id=d, device_id_type=MESH)

    def tables():
        lcol = jnp.broadcast_to(len_ref[...].astype(F32), (hd, n)).T
        ang = lcol * inv_ref[...]
        lane = lax.broadcasted_iota(jnp.int32, (n, hd), 1)
        cosb[...] = jnp.cos(ang)
        sn = jnp.sin(ang)
        sinb[...] = jnp.where(lane < hd // 2, -sn, sn)
        for g in range(grp):
            lrow[pl.ds(g, n, stride=grp), :] = lcol

    def remote(src, dst, ss, rs, dev):
        return pltpu.make_async_remote_copy(src_ref=src, dst_ref=dst, send_sem=ss, recv_sem=rs, device_id=dev,
                                            device_id_type=MESH)

    def halves(width):
        return [(k, k + LW) for k in range(0, width, LW)]

    def put_scale(row):
        rbuf[...] = jnp.broadcast_to(row, (LW, n)).T

    def local_scale():
        def sq(p, s):
            v = hbuf[p].astype(F32)
            return s + v * v
        s = lax.fori_loop(0, 2 * NB, sq, jnp.zeros((n, PW), F32))
        r = lax.rsqrt(jnp.sum(s, axis=-1, keepdims=True) * (1.0 / D) + EPS)
        rbuf[...] = jnp.broadcast_to(r, (n, LW))

    def normalize(l, ref, j):
        for h in range(2):
            p = j * 2 + h
            for a, b in halves(PW):
                g = ref[l:l + 1, cols(p * PW + a, LW)].astype(F32)
                abuf[p, :, a:b] = (hbuf[p, :, a:b].astype(F32) * rbuf[...] * g).astype(BF16)

    def group_dot(w, js, n0, nw):
        s = None
        for j in js:
            for h in range(2):
                d = _dot(abuf[j * 2 + h], w[rows(j * BW + h * PW, PW), n0:n0 + nw])
                s = d if s is None else s + d
        return s

    def unit(i):
        return pl.ds(i * n, n)

    def tiles(width):
        return [(n0, min(256, width - n0)) for n0 in range(0, width, 256)]

    def accumulate(u, d, first):
        for k, (a, b) in enumerate(halves(d.shape[1])):
            if first:
                pool[unit(u + k), :] = d[:, a:b]
            else:
                pool[unit(u + k), :] += d[:, a:b]

    UH = n // U
    slow = jnp.where(x == 0, 1, 0)
    SIDES = (slow, 1 - slow)
    right_i, left_i = right["tp"], left["tp"]

    def side_dev(h):
        return {"tp": jnp.where(h == 0, right_i, left_i)}

    def half_rows(u):
        return pl.ds(u * UH, UH)

    def reduce_scatter(block, wait_w, early, then):
        pair = []

        def other(i):
            j = (1 - c) * R + chip(RS_ORDER[i])
            o = block(j).astype(BF16)
            part[j, 0] = o[:, :PW]
            part[j, 1] = o[:, PW:]
            d = remote(part.at[j], pair_in.at[i], pr_s.at[i], pr_r.at[i], partner)
            d.start()
            pair.append(d)

        def mine(i):
            j = c * R + chip(RS_ORDER[i])
            o = block(j).astype(BF16)
            part[j, 0] = o[:, :PW]
            part[j, 1] = o[:, PW:]

        jo, jr, jl, jx = (c * R + chip(o) for o in RS_ORDER)
        m1 = [remote(part.at[jo, h, half_rows(u)], relay_in.at[h, half_rows(u)], rl_s.at[h * U + u],
                     rl_r.at[h * U + u], (right, left)[h]) for h in range(2) for u in range(U)]
        m2 = [remote(part.at[jr, 1], rs_in.at[0], rs_s.at[0], rs_r.at[0], right),
              remote(part.at[jl, 0], rs_in.at[1], rs_s.at[1], rs_r.at[1], left)]

        def opposite(k):
            for u in range(k * U // 2, (k + 1) * U // 2):
                for h in range(2):
                    ru = half_rows(u)
                    part[jo, h, ru] = (part[jo, h, ru].astype(F32) + pair_in[0, h, ru].astype(F32)).astype(BF16)
                    m1[h * U + u].start()

        def add_pair(i, j, hs):
            for h in hs:
                part[j, h] = (part[j, h].astype(F32) + pair_in[i, h].astype(F32)).astype(BF16)

        for j in range(NB):
            wait_w(j)
        with scope("rs_mm1"):
            other(0)
            other(1)
            if early:
                other(2)
            mine(0)
        with scope("rs_wait1"):
            pair[0].wait_recv()
            opposite(0)
            opposite(1)
        with scope("rs_mm2"):
            if not early:
                other(2)
            mine(1)
            mine(2)
        with scope("rs_send2"):
            pair[1].wait_recv()
            add_pair(1, jr, (1,))
            m2[0].start()
            pair[2].wait_recv()
            add_pair(2, jl, (0,))
            m2[1].start()
            add_pair(1, jr, (0,))
            add_pair(2, jl, (1,))
        with scope("rs_mm3"):
            other(3)
            mine(3)
            then()
        with scope("rs_relay"):
            m3 = []
            for u in range(U):
                for h in SIDES:
                    ru = half_rows(u)
                    j = jnp.where(h == 0, jr, jl)
                    remote(relay_in.at[h, ru], relay_in.at[h, ru], rl_s.at[h * U + u], rl_r.at[h * U + u], partner).wait_recv()
                    part[j, h, ru] = (part[j, h, ru].astype(F32) + relay_in[h, ru].astype(F32)).astype(BF16)
                    k = 2 + h * U + u
                    d = remote(part.at[j, h, ru], rs_in.at[2 + h, ru], rs_s.at[k], rs_r.at[k], side_dev(h))
                    d.start()
                    m3.append((h, u, d))
        own = (c * R + x) * 2
        with scope("rs_sum"):
            pair[3].wait_recv()
            for h in range(2):
                sown[h] = part[jx, h].astype(F32) + pair_in[3, h].astype(F32)
            for h in range(2):
                m2[1 - h].wait_recv()
                sown[h] = sown[h] + rs_in[1 - h].astype(F32)
        with scope("rs_fin"):
            first = []
            for h, u, d in m3:
                d.wait_recv()
                ru = half_rows(u)
                hbuf[own + h, ru] = (hbuf[own + h, ru].astype(F32) + (sown[h, ru] + rs_in[2 + h, ru].astype(F32))).astype(BF16)
                ref = hbuf.at[own + h, ru]
                k = h * U + u
                a = remote(ref, ref, ag_s.at[k], ag_r.at[k], side_dev(h))
                a.start()
                first.append((h, u, a))
        done = pair + m1 + m2 + [d for _, _, d in m3]
        return first, done

    def gather(first, done, stats, use):
        own = (c * R + x) * 2
        own2 = hbuf.at[pl.ds(own, 2)]
        p0 = remote(own2, own2, ad_s.at[0], ad_r.at[0], partner)
        p0.start()
        done = done + [p0]
        st = []
        with scope("stats"):
            if stats:
                q = None
                for h in range(2):
                    for a, b in halves(PW):
                        v = hbuf[own + h, :, a:b].astype(F32)
                        q = v * v if q is None else q + v * v
                sq = jnp.broadcast_to(jnp.sum(q.T, axis=0, keepdims=True), (8, n))
                stat[0] = sq
                for k in (4, 3, 5, 2, 6, 1, 7):
                    d = remote(stat.at[0], stat.at[k], st_s.at[k - 1], st_r.at[k - 1], peers[k - 1])
                    d.start()
                    st.append(d)
        with scope("ag_send2"):
            def piece(b, h):
                return hbuf.at[(c * R + b) * 2 + h]
            second = [remote(piece(x, 1), piece(x, 1), ag_s.at[2 * U], ag_r.at[2 * U], right),
                      remote(piece(x, 0), piece(x, 0), ag_s.at[2 * U + 1], ag_r.at[2 * U + 1], left)]
            for d in second:
                d.start()

        fw = []

        def forward(k, ref):
            d = remote(ref, ref, ad_s.at[k], ad_r.at[k], partner)
            d.start()
            fw.append(d)

        relay = []

        def both_cores(h, u, ref):
            k = h * U + u
            return remote(ref, ref, ax_s.at[k], ax_r.at[k], {"tp": side_dev(h)["tp"] + 1 - 2 * c})

        def last(h, u):
            return hbuf.at[(c * R + ob) * 2 + h, half_rows(u)]

        def last_forward(h, u):
            k = 3 + 2 * U + h * U + u
            return remote(last(h, u), last(h, u), ad_s.at[k], ad_r.at[k], partner)

        with scope("ag_relay"):
            for h, u, a in first:
                a.wait_recv()
                b = jnp.where(h == 0, lb, rb)
                ref = hbuf.at[(c * R + b) * 2 + h, half_rows(u)]
                k = 2 + 2 * U + h * U + u
                d = remote(ref, ref, ag_s.at[k], ag_r.at[k], side_dev(h))
                d.start()
                relay.append((h, u, d))
                forward(3 + h * U + u, ref)
                extra = both_cores(h, u, ref)

                @pl.when(c == 0)
                def _():
                    extra.start()
        with scope("ag_stats"):
            if stats:
                for d in st:
                    d.wait_recv()
                t = stat[0]
                for k in range(1, NB):
                    t = t + stat[k]
                put_scale(lax.rsqrt(t[0:1] * (1.0 / D) + EPS))
        with scope("use0"):
            p0.wait_recv()
            use(0)
        with scope("ag_2"):
            second[0].wait_recv()
            forward(1, piece(lb, 1))
            second[1].wait_recv()
            forward(2, piece(rb, 0))
        with scope("use1"):
            use(1)
        with scope("ag_3"):
            for h, u, d in relay:
                d.wait_recv()
                down = last_forward(h, u)

                @pl.when(c == 1)
                def _():
                    down.start()
        with scope("ag_fw1"):
            for d in fw:
                d.wait_recv()
        with scope("use2"):
            use(2)
        with scope("ag_fw2"):
            @pl.when(c == 0)
            def _():
                for h, u, _ in relay:
                    last_forward(h, u).wait_recv()

            @pl.when(c == 1)
            def _():
                for h, u, _ in relay:
                    both_cores(h, u, last(h, u)).wait_recv()
        with scope("use3"):
            use(3)
        with scope("ag_drain"):
            for d in done + [d for _, _, d in first + relay] + second + fw + st:
                d.wait_send()

            @pl.when(c == 1)
            def _():
                for h, u, _ in relay:
                    last_forward(h, u).wait_send()

            @pl.when(c == 0)
            def _():
                for h, u, _ in relay:
                    both_cores(h, u, last(h, u)).wait_send()

    def qkv_use(l):
        def use(g):
            js = GROUPS[g]
            for j in js:
                normalize(l, ga_ref, j)
            for j in js:
                cp_q(l, j).wait()
            for n0, nw in tiles(NQ):
                accumulate(5 * grp + n0 // LW, group_dot(wq, js, n0, nw), g == 0)
        return use

    quad_row = lax.broadcasted_iota(jnp.int32, (4 * grp, S), 0)
    low = quad_row < 2 * grp
    even = (quad_row // grp) % 2 == 0

    def four(s, t):
        a = kv[s, t:t + 2].reshape(2 * S, hd)
        b = kv[s, t + 2:t + 4].reshape(2 * S, hd)
        return jnp.concatenate([a, b], axis=1)

    scale = hd ** -0.5
    CH = NR // 4

    def attention(l):
        def rope(t):
            return (t * cosb[...] + pltpu.roll(t, hd // 2, 1) * sinb[...]).astype(BF16).astype(F32)

        def head(i):
            return pool[unit(5 * grp + i), :].astype(BF16).astype(F32)

        with scope("rope"):
            kn = rope(head(grp))
            vn = head(grp + 1)
            for g in range(grp):
                qrow[pl.ds(g, n, stride=grp), :] = rope(head(g))
                krow[pl.ds(g, n, stride=grp), :] = kn
                vrow[pl.ds(g, n, stride=grp), :] = vn

        with scope("qk"):
            for s in range(SLOTS):
                if s % SLOTS_PER_STEP == 0:
                    for s2 in range(s, s + SLOTS_PER_STEP):
                        cp_k(l, s2).wait()
                for t in range(0, T, 4):
                    r0 = (s * T + t) * grp
                    q4 = qrow[pl.ds(r0, 4 * grp), :]
                    q4 = jnp.concatenate([jnp.where(low, q4, 0.0), jnp.where(low, 0.0, q4)], axis=1).astype(BF16)
                    o = _dot_nt(q4, four(s, t))
                    arow[pl.ds(r0, 4 * grp), :] = jnp.where(even, o[:, :S], o[:, S:])
                cp_v(l, s).start()

        with scope("softmax"):
            for ch in range(4):
                rs = slice(ch * CH, (ch + 1) * CH)
                pos = lax.broadcasted_iota(jnp.int32, (CH, S), 1).astype(F32)
                sc = jnp.where(pos < lrow[rs, :], arow[rs, :] * scale, -jnp.inf)
                s_n = jnp.sum(qrow[rs, :] * krow[rs, :], axis=-1, keepdims=True) * scale
                m = jnp.maximum(jnp.max(sc, axis=-1, keepdims=True), s_n)
                p_c = jnp.exp(sc - m)
                p_n = jnp.exp(s_n - m)
                den = jnp.sum(p_c, axis=-1, keepdims=True) + p_n
                prow[rs, :] = p_c
                krow[rs, :] = jnp.broadcast_to(den, (CH, S))
                vrow[rs, :] = vrow[rs, :] * p_n

        with scope("pv"):
            for s in range(SLOTS):
                if s % SLOTS_PER_STEP == 0:
                    for s2 in range(s, s + SLOTS_PER_STEP):
                        cp_v(l, s2).wait()
                for t in range(0, T, 4):
                    r0 = (s * T + t) * grp
                    p4 = prow[pl.ds(r0, 4 * grp), :]
                    p4 = jnp.concatenate([jnp.where(even, p4, 0.0), jnp.where(even, 0.0, p4)], axis=1).astype(BF16)
                    o = _dot(p4, four(s, t))
                    arow[pl.ds(r0, 4 * grp), :] = jnp.where(low, o[:, :hd], o[:, hd:])

        with scope("att_out"):
            for ch in range(4):
                rs = slice(ch * CH, (ch + 1) * CH)
                arow[rs, :] = (arow[rs, :] + vrow[rs, :]) / krow[rs, :]
            for g in range(grp):
                att[:, g * hd:(g + 1) * hd] = arow[pl.ds(g, n, stride=grp), :].astype(BF16)

    def mlp_use(l):
        FU = F // LW

        def use(g):
            js = GROUPS[g]
            for j in js:
                normalize(l, gm_ref, j)
            for j in js:
                cp_g(l, j).wait()
                cp_u(l, j).wait()
            for n0, nw in tiles(F):
                if g < NG - 1:
                    for k, w in enumerate((wg, wu)):
                        accumulate((k * F + n0) // LW, group_dot(w, js, n0, nw), g == 0)
                else:
                    dg, du = group_dot(wg, js, n0, nw), group_dot(wu, js, n0, nw)
                    for k, (a, b) in enumerate(halves(nw)):
                        u = n0 // LW + k
                        gate = pool[unit(u), :] + dg[:, a:b]
                        up = pool[unit(FU + u), :] + du[:, a:b]
                        act[:, n0 + a:n0 + b] = (jax.nn.silu(gate) * up).astype(BF16)
        return use

    with scope("x_wait"):
        for p in range(2 * NB):
            cp_x(p).wait()
    with scope("scale0"):
        for j in blocks[4:]:
            cp_q(0, j).start()
        for s in range(SLOTS // 2):
            cp_k(0, s).start()
        local_scale()
        for d in small:
            d.wait()

    outs = []

    def out_use(g):
        for j in GROUPS[g]:
            for h in range(2):
                p = j * 2 + h
                d = pltpu.make_async_copy(hbuf.at[p], y_hbm.at[:, cols(p * PW, PW)], s_y.at[g * 4 + len(outs) % 4])
                d.start()
                outs.append(d)

    pending = None
    for l in range(L):
        if pending is None:
            for g in range(NG):
                with scope("qkv"):
                    qkv_use(l)(g)
                if g == 0:
                    with scope("tables"):
                        tables()
                if g == 0:
                    for s in range(SLOTS // 2, SLOTS):
                        cp_k(0, s).start()
                if g == 2:
                    for j in range(NB):
                        cp_o(0, j).start()
        else:
            gather(*pending, True, qkv_use(l))
        attention(l)
        if l == 0:
            pl.semaphore_wait(barrier, NB - 1)

        def mlp_weights(l=l):
            if l == 0:
                for j in blocks:
                    cp_g(0, j).start()
                    cp_u(0, j).start()
                for j in range(NB):
                    cp_d(0, j).start()

        pending = reduce_scatter(lambda j: _dot(att[...], wo[:, cols(j * BW, BW)]), lambda j: cp_o(l, j).wait(), True, mlp_weights)
        if l + 1 < L:
            for j in range(NB):
                cp_o(l + 1, j).start()
        gather(*pending, True, mlp_use(l))
        if l + 1 < L:
            for j in blocks:
                cp_q(l + 1, j).start()
            for s in range(SLOTS):
                cp_k(l + 1, s).start()
            for j in blocks:
                cp_g(l + 1, j).start()
                cp_u(l + 1, j).start()
        pending = reduce_scatter(lambda j: _dot(act[...], wd[:, cols(j * BW, BW)]), lambda j: cp_d(l, j).wait(), False, lambda: None)
        if l + 1 < L:
            for j in range(NB):
                cp_d(l + 1, j).start()
    gather(*pending, False, out_use)
    with scope("y_out"):
        for d in outs:
            d.wait()


def solution(mesh):
    tp = mesh.shape["tp"]

    def body(x, g_attn, w_qkv, w_o, g_mlp, w_gate, w_up, w_down, k_cache, v_cache, lengths):
        n, D = x.shape
        L, _, NQ = w_qkv.shape
        KO, F = w_o.shape[1], w_gate.shape[2]
        S, hd = k_cache.shape[2], k_cache.shape[4]
        R = tp // 2
        NB, PW, BW = tp, D // tp // 2, D // tp
        grp = KO // hd
        kc = k_cache.reshape(L, n, S, hd)
        vc = v_cache.reshape(L, n, S, hd)
        half = hd // 2
        inv = np.float32(ROPE_THETA) ** (-np.arange(half, dtype=np.float32) * np.float32(2.0) / np.float32(hd))
        inv = jnp.asarray(np.concatenate([inv, inv])[None, :].astype(np.float32))
        dims = (L, n, D, NQ, KO, F, S, hd, R)
        anyspec = pl.BlockSpec(memory_space=pl.ANY)
        V = pltpu.VMEM
        DMA = pltpu.SemaphoreType.DMA
        rows = n * grp
        scratch = [
            V((D, NQ), BF16), V((KO, D), BF16), V((D, F), BF16), V((D, F), BF16), V((F, D), BF16),
            V((SLOTS, n // SLOTS, S, hd), BF16),
            V((2 * NB, n, PW), BF16), V((2 * NB, n, PW), BF16),
            V((NB, 2, n, PW), BF16), V((R, 2, n, PW), BF16), V((2, n, PW), BF16), V((4, n, PW), BF16), V((2, n, PW), F32),
            V((max(2 * F // 128, 5 * grp + NQ // 128) * n, 128), F32), V((n, F), BF16),
            V((rows, hd), F32), V((n, hd), F32), V((n, hd), F32), V((n, KO), BF16), V((n, 128), F32), V((NB, 8, n), F32),
            V((L, D), BF16), V((L, D), BF16), V((1, n), jnp.int32), V((1, hd), F32), DMA((4,)),
            DMA((2 * NB,)), DMA((NB,)), DMA((NB,)), DMA((NB,)), DMA((NB,)), DMA((NB,)), DMA((SLOTS,)), DMA((2 * NB,)),
            DMA((4,)), DMA((4,)), DMA((2 * U,)), DMA((2 * U,)), DMA((2 + 2 * U,)), DMA((2 + 2 * U,)),
            DMA((2 + 4 * U,)), DMA((2 + 4 * U,)), DMA((3 + 4 * U,)), DMA((3 + 4 * U,)), DMA((2 * U,)), DMA((2 * U,)),
            DMA((NB - 1,)), DMA((NB - 1,)),
        ]
        y = pl.pallas_call(
            functools.partial(_kernel, dims),
            out_shape=jax.ShapeDtypeStruct((n, D), BF16),
            in_specs=[anyspec] * 12,
            out_specs=anyspec,
            scratch_shapes=scratch,
            compiler_params=pltpu.CompilerParams(collective_id=0, has_side_effects=True, vmem_limit_bytes=67043328),
        )(x, g_attn, w_qkv, w_o, g_mlp, w_gate, w_up, w_down, kc, vc, lengths.reshape(1, n), inv)
        return y

    col = P(None, None, 'tp')
    row = P(None, 'tp', None)
    cache = P(None, 'dp', None, 'tp', None)
    return jax.shard_map(body, mesh=mesh,
                         in_specs=(P('dp', None), P(), col, row, P(), col, col, row, cache, cache, P('dp')),
                         out_specs=P('dp', None), check_vma=False)
```
